32 devices in a mesh: dp: 2 (over x), row: 4 (over z), col: 4 (over y, core).
Axes of the slice: x: 2, y: 2, z: 4, core: 2. Of those that a mesh axis runs over, the one named last changes fastest.
Arguments:
- x: bfloat16 [2, 32, 512, 2048], P(None, ('dp', 'row', 'col')), parts along dimension 1
- idx: int32 [2, 32, 512, 6], P(None, ('dp', 'row', 'col')), parts along dimension 1
- gates: float32 [2, 32, 512, 6], P(None, ('dp', 'row', 'col')), parts along dimension 1
- wq: bfloat16 [2048, 2048], replicated
- wk: bfloat16 [2048, 2048], replicated
- wv: bfloat16 [2048, 2048], replicated
- wo: bfloat16 [2048, 2048], replicated
- gattn: float32 [2048], replicated
- gmoe: float32 [2048], replicated
- w1: bfloat16 [64, 2048, 1408], P(('row', 'col'))
- w3: bfloat16 [64, 2048, 1408], P(('row', 'col'))
- w2: bfloat16 [64, 1408, 2048], P(('row', 'col'))
Outputs:
- output: bfloat16 [2, 32, 512, 2048], P(None, ('dp', 'row', 'col')), parts along dimension 1
There are 2 independent parts. The reference program is written for one: setup_inputs(seed, part) draws one part's arguments, and reference() takes and returns one part's arrays. A program takes and returns all parts, laid end to end along the dimension named above; an argument that names none is the same for every part.
All inputs are finite; a program needn't handle non-finite values.
Results may differ from the reference program's by a relative error of at most 0.00883776.
Values are sent between devices in bfloat16 or wider.
A program may use at most 1 GiB of HBM per device.

```python
import jax
import jax.numpy as jnp
from jax import lax

D = 2048
HEADS = 16
HEAD = 128
EXPERTS = 64
TOP = 6
FF = 1408
TOKENS = 512
SEQ = 512
GROUP = 16

CAP = ((TOP * ((2 * TOKENS + EXPERTS - 1) // EXPERTS) + 7) // 8) * 8
NTOK = GROUP * TOKENS
NSEQ = NTOK // SEQ


def draw_routing(key):
    k1, k2, k3 = jax.random.split(key, 3)
    k1 = jax.random.fold_in(k1, 7919)
    k2 = jax.random.fold_in(k2, 7919)
    offset = jax.random.randint(k1, (), 0, EXPERTS)
    ranks = jax.vmap(lambda kk: jax.random.permutation(kk, TOKENS))(jax.random.split(k2, GROUP))
    half = TOKENS // 2
    quarter = EXPERTS // 4
    r = jnp.where(ranks < half, (ranks * quarter) // half, quarter + ((ranks - half) * (EXPERTS - quarter)) // half)
    pos = (offset + r[:, :, None] - jnp.arange(TOP)[None, None, :]) % EXPERTS
    idx = pos.reshape(NSEQ, SEQ, TOP).astype(jnp.int32)
    gates = jax.nn.softmax(jax.random.normal(k3, (NSEQ, SEQ, TOP), jnp.float32), axis=-1)
    return idx, gates


def setup_inputs(seed: int = 0, part: int = 0) -> dict:
    key = jax.random.key(seed)
    kw = jax.random.split(key, 10)
    kp = jax.random.split(jax.random.fold_in(key, part), 4)
    hd = HEADS * HEAD
    base = jax.random.normal(kp[0], (2, NSEQ, SEQ, D), jnp.float32)
    shift = 0.8 * jax.random.normal(kp[1], (2, NSEQ, 1, D), jnp.float32)
    x = (base + shift).astype(jnp.bfloat16)
    ia, ga = draw_routing(kp[2])
    ib, gb = draw_routing(kp[3])
    idx = jnp.stack([ia, ib])
    gates = jnp.stack([ga, gb])
    wq = (jax.random.normal(kw[0], (D, hd), jnp.float32) * D ** -0.5).astype(jnp.bfloat16)
    wk = (jax.random.normal(kw[1], (D, hd), jnp.float32) * D ** -0.5).astype(jnp.bfloat16)
    wv = (jax.random.normal(kw[2], (D, hd), jnp.float32) * D ** -0.5).astype(jnp.bfloat16)
    wo = (jax.random.normal(kw[3], (hd, D), jnp.float32) * hd ** -0.5).astype(jnp.bfloat16)
    gattn = 1.0 + 0.3 * jax.random.normal(kw[4], (D,), jnp.float32)
    gmoe = 1.0 + 0.3 * jax.random.normal(kw[5], (D,), jnp.float32)
    w1 = (jax.random.normal(kw[6], (EXPERTS, D, FF), jnp.float32) * D ** -0.5).astype(jnp.bfloat16)
    w3 = (jax.random.normal(kw[7], (EXPERTS, D, FF), jnp.float32) * D ** -0.5).astype(jnp.bfloat16)
    w2 = (jax.random.normal(kw[8], (EXPERTS, FF, D), jnp.float32) * 2.0 * FF ** -0.5).astype(jnp.bfloat16)
    return {"x": x, "idx": idx, "gates": gates, "wq": wq, "wk": wk, "wv": wv, "wo": wo, "gattn": gattn, "gmoe": gmoe, "w1": w1, "w3": w3, "w2": w2}


def rms(v, g):
    vf = v.astype(jnp.float32)
    return (vf * lax.rsqrt(jnp.mean(vf * vf, axis=-1, keepdims=True) + 1e-6) * g).astype(jnp.bfloat16)


def attention(x, wq, wk, wv, wo, gattn):
    u = rms(x, gattn)

    def proj(w):
        a = jnp.dot(u, w, preferred_element_type=jnp.float32).astype(jnp.bfloat16)
        return a.reshape(NSEQ, SEQ, HEADS, HEAD).transpose(2, 0, 1, 3)

    q, k, v = proj(wq), proj(wk), proj(wv)
    causal = jnp.arange(SEQ)[:, None] >= jnp.arange(SEQ)[None, :]

    def one_head(qkv):
        qh, kh, vh = qkv
        s = jnp.einsum("cre,cle->crl", qh.astype(jnp.float32), kh.astype(jnp.float32)) * HEAD ** -0.5
        s = jnp.where(causal[None], s, -1e30)
        p = jax.nn.softmax(s, axis=-1).astype(jnp.bfloat16)
        o = jnp.einsum("crl,cle->cre", p.astype(jnp.float32), vh.astype(jnp.float32))
        return o.astype(jnp.bfloat16)

    o = lax.map(one_head, (q, k, v))
    o = o.transpose(1, 2, 0, 3).reshape(NTOK, HEADS * HEAD)
    a = jnp.dot(o, wo, preferred_element_type=jnp.float32)
    return (x.astype(jnp.float32) + a).astype(jnp.bfloat16)


def moe(h, idx, gates, w1, w3, w2, gmoe):
    z = rms(h, gmoe)
    zpad = jnp.concatenate([z, jnp.zeros((1, D), jnp.bfloat16)], axis=0)
    flat = idx.reshape(-1)
    gflat = gates.reshape(-1)
    order = jnp.argsort(flat, stable=True)
    counts = jnp.zeros((EXPERTS,), jnp.int32).at[flat].add(1)
    starts = jnp.cumsum(counts) - counts
    width = GROUP * CAP

    def step(acc, per_expert):
        a1, a3, a2, st, ct = per_expert
        slot = st + jnp.arange(width)
        valid = slot < st + ct
        pair = order[jnp.minimum(slot, NTOK * TOP - 1)]
        tok = jnp.where(valid, pair // TOP, NTOK)
        gate = jnp.where(valid, gflat[pair], 0.0)
        rows = zpad[tok]
        h1 = jnp.dot(rows, a1, preferred_element_type=jnp.float32)
        h3 = jnp.dot(rows, a3, preferred_element_type=jnp.float32)
        act = (jax.nn.silu(h1) * h3).astype(jnp.bfloat16)
        out = jnp.dot(act, a2, preferred_element_type=jnp.float32).astype(jnp.bfloat16)
        acc = acc.at[tok].add(gate[:, None] * out.astype(jnp.float32), mode="drop")
        return acc, None

    acc, _ = lax.scan(step, jnp.zeros((NTOK, D), jnp.float32), (w1, w3, w2, starts, counts))
    return (h.astype(jnp.float32) + acc).astype(jnp.bfloat16)


def reference(x, idx, gates, wq, wk, wv, wo, gattn, gmoe, w1, w3, w2):
    ys = []
    for m in range(2):
        h = attention(x[m].reshape(NTOK, D), wq, wk, wv, wo, gattn)
        y = moe(h, idx[m].reshape(NTOK, TOP), gates[m].reshape(NTOK, TOP), w1, w3, w2, gmoe)
        ys.append(y.reshape(NSEQ, SEQ, D))
    return jnp.stack(ys)
```

```python
import functools

import jax
import jax.numpy as jnp
from jax import lax
from jax.experimental import pallas as pl
from jax.experimental.pallas import tpu as pltpu
from jax.sharding import PartitionSpec as P

HEAD = 128
LANES = 128
TILE = 128
GRAIN = 16
WIDTH = 288
SINGLE = False
NONE = -(1 << 20)
F32, BF16, I32 = jnp.float32, jnp.bfloat16, jnp.int32
ANY = pl.BlockSpec(memory_space=pl.ANY)
SMEM = pl.BlockSpec(memory_space=pltpu.SMEM)
VMEM = pl.BlockSpec(memory_space=pltpu.VMEM)
CORE_SWAP = [(0, 1), (1, 0), (2, 3), (3, 2)]
CHIP_SWAP = [(0, 2), (1, 3), (2, 0), (3, 1)]


def rms(v, g):
    vf = v.astype(F32)
    return (vf * lax.rsqrt(jnp.mean(vf * vf, axis=-1, keepdims=True) + 1e-6) * g).astype(BF16)


def attention(x, wq, wk, wv, wo, g):
    ns, seq, d = x.shape
    nh = wq.shape[1] // HEAD
    xf = x.reshape(ns * seq, d)
    u = rms(xf, g)

    def proj(w):
        a = jnp.dot(u, w, preferred_element_type=F32).astype(BF16)
        return a.reshape(ns, seq, nh, HEAD)

    q, k, v = proj(wq), proj(wk), proj(wv)
    causal = jnp.arange(seq)[:, None] >= jnp.arange(seq)[None, :]
    s = jnp.einsum("bqhe,bkhe->bhqk", q, k, preferred_element_type=F32) * HEAD ** -0.5
    s = jnp.where(causal, s, -1e30)
    p = jax.nn.softmax(s, axis=-1).astype(BF16)
    o = jnp.einsum("bhqk,bkhe->bqhe", p, v, preferred_element_type=F32).astype(BF16)
    a = jnp.dot(o.reshape(ns * seq, nh * HEAD), wo, preferred_element_type=F32)
    return (xf.astype(F32) + a).astype(BF16)


def capacity(t, top, n_exp):
    return ((top * ((2 * t + n_exp - 1) // n_exp) + 7) // 8) * 8


def split3(v):
    a = v.astype(BF16)
    r = v - a.astype(F32)
    b = r.astype(BF16)
    return a, b, (r - b.astype(F32)).astype(BF16)


def ranks(hit):
    t = hit.shape[-1]
    tri = (jnp.arange(t)[:, None] < jnp.arange(t)[None, :]).astype(BF16)
    n = jnp.dot(hit.reshape(-1, t).astype(BF16), tri, preferred_element_type=F32).astype(I32)
    return jnp.where(hit, n.reshape(hit.shape), NONE)


def among(idx, first, n):
    e = first + jnp.arange(n, dtype=I32)
    return idx[:, :, None, :] == e[None, None, :, None]


def expert_kernel(cap, tok, meta, pos, z, w1, w3, w2, oa, ob, done, zb, x, act, w13b, w2b, zs, ws, os):
    el, d, f = w1.shape
    ns = pos.shape[0] // el
    t = z.shape[1]
    fb, nb = f // LANES, d // LANES
    outs = [(oa if i < ns // 2 else ob).at[i % (ns // 2)] for i in range(ns)]

    def off(i, e):
        return pl.multiple_of(meta[ns + i * el + e], GRAIN)

    def fetch(i):
        return pltpu.make_async_copy(z.at[meta[i]], zb.at[i % 2], zs.at[i % 2])

    def put(i, e):
        return pltpu.make_async_copy(x.at[e, pl.ds(off(i, e), cap)], outs[i].at[pl.ds(e * cap, cap)], os.at[i * el + e])

    def weights(e):
        s = e % 2
        cs = []
        for i in range(fb):
            for o, w in enumerate((w1, w3)):
                cs.append(pltpu.make_async_copy(w.at[e, :, pl.ds(i * LANES, LANES)],
                                                w13b.at[s, :, pl.ds((2 * i + o) * LANES, LANES)],
                                                ws.at[s, 2 * i + o]))
        cs.append(pltpu.make_async_copy(w2.at[e], w2b.at[s], ws.at[s, 2 * fb]))
        return cs

    fetch(0).start()
    fetch(1).start()
    for e in range(2):
        for c in weights(e):
            c.start()
    for i in range(ns):
        fetch(i).wait()
        row = lax.broadcasted_iota(I32, (cap, t), 0)
        sel = jnp.concatenate([jnp.where(row == pos[i * el + e:i * el + e + 1, :], 1.0, 0.0).astype(BF16) for e in range(el)], 0)
        for c in range(4):
            cols = slice(c * d // 4, (c + 1) * d // 4)
            v = jnp.dot(sel, zb[i % 2, :, cols], preferred_element_type=F32).astype(BF16)
            for e in range(el):
                x[e, pl.ds(off(i, e), cap), cols] = v[e * cap:(e + 1) * cap]
        if i + 2 < ns:
            fetch(i + 2).start()

    for e in range(el):
        s = e % 2
        for c in weights(e):
            c.wait()

        def tile(i, carry, e=e, s=s):
            rows = pl.ds(pl.multiple_of(i * TILE, TILE), TILE)
            for c in range(fb):
                h = jnp.dot(x[e, rows, :], w13b[s, :, 2 * c * LANES:2 * (c + 1) * LANES], preferred_element_type=F32)
                act[:, c * LANES:(c + 1) * LANES] = (jax.nn.silu(h[:, :LANES]) * h[:, LANES:]).astype(BF16)
            for c in range(nb // 2):
                cols = slice(2 * c * LANES, 2 * (c + 1) * LANES)
                x[e, rows, cols] = jnp.dot(act[...], w2b[s, :, cols], preferred_element_type=F32).astype(BF16)
            return carry
        lax.fori_loop(0, meta[ns + ns * el + e], tile, 0)
        for i in range(ns):
            put(i, e).start()
        if e + 2 < el:
            for c in weights(e + 2):
                c.start()
    for e in range(el):
        for i in range(ns):
            put(i, e).wait()


def combine_kernel(cap, tok, pos, gate, ea, eb, *refs):
    *outs, done, buf, ob, es, os = refs
    ns = len(outs)
    d = outs[0].shape[1]
    n = pos.shape[0] // ns
    width = pos.shape[1]
    rows = ea.shape[1]

    def fetch(i):
        return (pltpu.make_async_copy(ea.at[i], buf.at[i % 2, pl.ds(0, rows)], es.at[i % 2, 0]),
                pltpu.make_async_copy(eb.at[i], buf.at[i % 2, pl.ds(rows, rows)], es.at[i % 2, 1]))

    def put(i):
        return pltpu.make_async_copy(ob.at[i % 2], outs[i], os.at[i % 2])

    for i in range(ns):
        for c in fetch(i):
            c.start()
    for i in range(ns):
        s = i % 2
        row = lax.broadcasted_iota(I32, (cap, width), 0)
        m = jnp.concatenate([jnp.where(row == pos[i * n + e:i * n + e + 1, :], gate[i * n + e:i * n + e + 1, :], 0.0)
                             for e in range(n)], 0)
        parts = split3(m)
        for c in fetch(i):
            c.wait()
        for c in range(4):
            cols = slice(c * d // 4, (c + 1) * d // 4)
            a = [lax.dot_general(p, buf[s, :, cols], (((0,), (0,)), ((), ())), preferred_element_type=F32) for p in parts]
            ob[s, :, cols] = a[0] + a[1] + a[2]
        put(i).start()
    for i in range(ns):
        put(i).wait()


def add_kernel(tok, a, b, o, done):
    o[...] = a[...] + b[...]


def sum_kernel(tok, pos, h, *refs):
    first, second, *rest, y, done = refs
    nl = len(rest) + 1
    width, d = first.shape
    t = h.shape[0]
    lane = lax.broadcasted_iota(I32, (t, width), 1)
    hot = [jnp.where(lane == pos[:, l:l + 1], 1.0, 0.0).astype(BF16) for l in range(nl)]
    for c in range(8):
        cols = slice(c * d // 8, (c + 1) * d // 8)
        a = h[:, cols].astype(F32)
        for l in range(nl):
            v = first[:, cols] + second[:, cols] if l == 0 else rest[l - 1][:, cols]
            for p in split3(v):
                a = a + jnp.dot(hot[l], p, preferred_element_type=F32)
        y[:, cols] = a.astype(BF16)


def solution(mesh):
    ep_axes = ("row", "col")
    tok_axes = ("dp", "row", "col")
    nrow, ncol = mesh.shape["row"], mesh.shape["col"]
    ep = nrow * ncol

    def local(x, idx, gates, wq, wk, wv, wo, gattn, gmoe, w1, w3, w2):
        nm, ns, seq, d = x.shape
        t = ns * seq
        top = idx.shape[-1]
        el, _, f = w1.shape
        n_exp = el * ep
        layer = n_exp // nrow
        cap = capacity(t, top, n_exp)
        params = functools.partial(pltpu.CompilerParams, vmem_limit_bytes=67043328)
        cost = lambda n, b: pl.CostEstimate(flops=n, bytes_accessed=b, transcendentals=0)
        row, col = lax.axis_index("row"), lax.axis_index("col")
        me = row * ncol + col
        chip, core = col // 2, col % 2
        tok0 = jnp.zeros((8, LANES), I32)
        token = jax.ShapeDtypeStruct((8, LANES), I32)

        pay = jnp.concatenate([idx.astype(F32), gates, jnp.zeros((nm, ns, seq, 16 - 2 * top), F32)], -1)
        pay = jnp.swapaxes(pay.reshape(nm, t, 16), 1, 2)
        every = lax.all_gather(pay, tok_axes)
        every = every.reshape((-1, ep) + every.shape[1:])

        def width_needed():
            rows_of = every[:, :, :, :top] // layer
            hit = jnp.any(rows_of[..., None] == jnp.arange(nrow, dtype=F32), axis=3)
            return jnp.max(jnp.sum(hit.astype(I32), axis=3))

        need = width_needed()
        mine = lax.dynamic_index_in_dim(every, lax.axis_index("dp"), 0, keepdims=False)

        def flip(a, axis, bit):
            return jnp.where(bit == 0, jnp.flip(a, axis), a)

        def relative(a):
            a = a.reshape((nrow, 2, 2) + a.shape[1:])
            a = lax.dynamic_slice_in_dim(jnp.concatenate([a, a]), row, nrow)
            return flip(flip(jnp.swapaxes(a, 1, 2), 1, core), 2, chip)

        def routes(m, width):
            ia = relative(mine[:, m, :top].astype(I32))
            ga = relative(mine[:, m, top:2 * top])
            src = relative(jnp.arange(ep, dtype=I32)).reshape(nrow, 4)
            flat = lambda a: a.reshape((-1,) + a.shape[3:])
            pos = ranks(jnp.any(among(flat(ia), me * el, el), 1)).reshape(nrow, 4, el, t)
            cnt = jnp.maximum(jnp.max(pos, -1) + 1, 0)
            seg = (cnt + GRAIN - 1) // GRAIN * GRAIN
            before = jnp.arange(4)[:, None] > jnp.arange(4)[None, :]
            offs = jnp.sum(jnp.where(before[None, :, :, None], seg[:, None], 0), 2)
            tiles = (jnp.sum(seg, 1) + TILE - 1) // TILE
            meta = jnp.concatenate([src, offs.reshape(nrow, -1), tiles], 1)
            ik, gk = ia[:, 1].reshape(nrow * 2, top, t), ga[:, 1].reshape(nrow * 2, top, t)
            hits = among(ik, 2 * el * (me // 2), 2 * el)
            pos8 = ranks(jnp.any(hits, 1))
            g8 = jnp.sum(jnp.where(hits, gk[:, :, None, :], 0.0), 1)
            listed = ranks(jnp.any(ik // layer == row, 1))
            lists = (listed[:, :, None] == jnp.arange(width, dtype=I32)).astype(BF16)
            cols = jnp.concatenate([(jnp.maximum(pos8, -1) + 1).astype(BF16)] + list(split3(g8)), 1)
            byrow = jnp.einsum("pet,ptc->pec", cols, lists, preferred_element_type=F32)
            k = 2 * el
            lpos = byrow[:, :k].astype(I32) - 1
            lgate = byrow[:, k:2 * k] + byrow[:, 2 * k:3 * k] + byrow[:, 3 * k:]
            turn = lambda a: jnp.where(core == 0, a, jnp.roll(a, el, axis=1)).reshape(nrow, 2 * k, width)
            steps = lax.rem(row + nrow - jnp.arange(nrow, dtype=I32), nrow)
            home = ranks(jnp.any(idx[m].reshape(1, t, top) // layer == steps[:, None, None], 2))
            home = jnp.pad(home.T, ((0, 0), (0, LANES - nrow)))
            return pos.reshape(nrow, 4 * el, t), meta, turn(lpos), turn(lgate), home

        def experts(tok, r, pos, meta, za):
            out = jax.ShapeDtypeStruct((2, el * cap, d), BF16)
            *outs, tok = pl.pallas_call(
                functools.partial(expert_kernel, cap), out_shape=[out, out, token],
                in_specs=[ANY, SMEM, VMEM] + [ANY] * 4, out_specs=[ANY] * 3,
                scratch_shapes=[
                    pltpu.VMEM((2, t, d), BF16),
                    pltpu.VMEM((el, -(-5 * cap // TILE) * TILE, d), BF16),
                    pltpu.VMEM((TILE, f), BF16),
                    pltpu.VMEM((2, d, 2 * f), BF16),
                    pltpu.VMEM((2, f, d), BF16),
                    pltpu.SemaphoreType.DMA((2,)),
                    pltpu.SemaphoreType.DMA((2, 2 * (f // LANES) + 1)),
                    pltpu.SemaphoreType.DMA((4 * el,)),
                ],
                compiler_params=params(), name="experts", cost_estimate=cost(35_000_000_000, 80_000_000),
            )(tok, meta[r], pos[r], za, w1, w3, w2)
            return outs, tok

        def combine(tok, r, lpos, lgate, ea, eb):
            width = lpos.shape[-1]
            out = jax.ShapeDtypeStruct((width, d), F32)
            *outs, tok = pl.pallas_call(
                functools.partial(combine_kernel, cap), out_shape=[out, out, token],
                in_specs=[ANY, VMEM, VMEM, ANY, ANY], out_specs=[ANY] * 3,
                scratch_shapes=[
                    pltpu.VMEM((2, 2 * el * cap, d), BF16),
                    pltpu.VMEM((2, width, d), F32),
                    pltpu.SemaphoreType.DMA((2, 2)),
                    pltpu.SemaphoreType.DMA((2,)),
                ],
                compiler_params=params(), name="combine", cost_estimate=cost(8_000_000_000, 11_000_000),
            )(tok, lpos[r], lgate[r], ea, eb)
            return outs, tok

        def add(tok, a, b):
            width = a.shape[0]
            block = pl.BlockSpec((width // 4, d), lambda i: (i, 0))
            return pl.pallas_call(
                add_kernel, grid=(4,), out_shape=[jax.ShapeDtypeStruct(a.shape, F32), token],
                in_specs=[ANY, block, block], out_specs=[block, ANY], name="add_rows",
                compiler_params=params(), cost_estimate=cost(3_000_000_000, 7_000_000),
            )(tok, a, b)

        def total(tok, home, h, parts):
            y, tok = pl.pallas_call(
                sum_kernel, out_shape=[jax.ShapeDtypeStruct((t, d), BF16), token],
                in_specs=[ANY] + [VMEM] * (2 + len(parts)), out_specs=[VMEM, ANY], name="sum_rows",
                compiler_params=params(), cost_estimate=cost(10_000_000_000, 16_000_000),
            )(tok, home, h, *parts)
            return y, tok

        def layers(width, h0, z0, x):
            za, hs = [lax.all_gather(z0, ep_axes).reshape(ep, t, d)], [h0]
            x1, _ = lax.optimization_barrier((x[1], z0))
            hs.append(attention(x1, wq, wk, wv, wo, gattn))
            za.append(lax.all_gather(rms(hs[1], gmoe), ep_axes).reshape(ep, t, d))
            rt = [routes(m, width) for m in range(nm)]
            tok = tok0
            mineE, inE, mineP, inP, got = {}, {}, {}, {}, {}
            ys = []
            plan = ["X02", "X01", "B02", "X03", "B01", "A02", "X00", "B03", "A01",
                    "X12", "B00", "A03", "X11", "B12", "X13", "B11", "A12", "X10", "B13", "A11", "F0", "B10", "A13", "F1"]
            for step in plan:
                op, m = step[0], int(step[1])
                pos, meta, lpos, lgate, home = rt[m]
                key = step[1:]
                if op == "X":
                    (other, mineE[key]), tok = experts(tok, int(step[2]), pos, meta, za[m])
                    inE[key] = lax.ppermute(other, "col", CORE_SWAP)
                elif op == "B":
                    (other, mineP[key]), tok = combine(tok, int(step[2]), lpos, lgate, mineE[key], inE[key])
                    inP[key] = lax.ppermute(other, "col", CHIP_SWAP)
                elif op == "A":
                    r = int(step[2])
                    s, tok = add(tok, mineP[key], inP[key])
                    got[key] = lax.ppermute(s, "row", [(i, (i + r) % nrow) for i in range(nrow)])
                else:
                    k = str(m) + "0"
                    y, tok = total(tok, home, hs[m], [mineP[k], inP[k]] + [got[str(m) + str(r)] for r in range(1, nrow)])
                    ys.append(y)
            return jnp.stack(ys).reshape(nm, ns, seq, d)

        h0 = attention(x[0], wq, wk, wv, wo, gattn)
        z0 = rms(h0, gmoe)
        if SINGLE:
            return layers(WIDTH, h0, z0, x)
        return lax.cond(need <= WIDTH, functools.partial(layers, WIDTH), functools.partial(layers, t), h0, z0, x)

    tok_spec = P(None, tok_axes)
    exp_spec = P(ep_axes)
    return jax.shard_map(local, mesh=mesh,
                         in_specs=(tok_spec, tok_spec, tok_spec, P(), P(), P(), P(), P(), P(), exp_spec, exp_spec, exp_spec),
                         out_specs=tok_spec, check_vma=False)
```

```python
import functools

import jax
import jax.numpy as jnp
from jax import lax
from jax.experimental import pallas as pl
from jax.experimental.pallas import tpu as pltpu
from jax.sharding import PartitionSpec as P

HEAD = 128
LANES = 128
TILE = 128
GRAIN = 16
WIDTH = 288
SINGLE = False
PLAN = ("X00", "X01", "B00", "X03", "B01", "W00", "X02", "B03", "A01", "X12", "B02", "A03", "X11", "W01", "B12",
        "A02", "X13", "W03", "B11", "A12", "X10", "W02", "B13", "A11", "F0", "W12", "B10", "A13", "F1")
NONE = -(1 << 20)
F32, BF16, I32 = jnp.float32, jnp.bfloat16, jnp.int32
ANY = pl.BlockSpec(memory_space=pl.ANY)
SMEM = pl.BlockSpec(memory_space=pltpu.SMEM)
VMEM = pl.BlockSpec(memory_space=pltpu.VMEM)
CORE_SWAP = [(0, 1), (1, 0), (2, 3), (3, 2)]
CHIP_SWAP = [(0, 2), (1, 3), (2, 0), (3, 1)]


def rms(v, g):
    vf = v.astype(F32)
    return (vf * lax.rsqrt(jnp.mean(vf * vf, axis=-1, keepdims=True) + 1e-6) * g).astype(BF16)


def attention(x, wq, wk, wv, wo, g):
    ns, seq, d = x.shape
    nh = wq.shape[1] // HEAD
    xf = x.reshape(ns * seq, d)
    u = rms(xf, g)

    def proj(w):
        a = jnp.dot(u, w, preferred_element_type=F32).astype(BF16)
        return a.reshape(ns, seq, nh, HEAD)

    q, k, v = proj(wq), proj(wk), proj(wv)
    causal = jnp.arange(seq)[:, None] >= jnp.arange(seq)[None, :]
    s = jnp.einsum("bqhe,bkhe->bhqk", q, k, preferred_element_type=F32) * HEAD ** -0.5
    s = jnp.where(causal, s, -1e30)
    p = jax.nn.softmax(s, axis=-1).astype(BF16)
    o = jnp.einsum("bhqk,bkhe->bqhe", p, v, preferred_element_type=F32).astype(BF16)
    a = jnp.dot(o.reshape(ns * seq, nh * HEAD), wo, preferred_element_type=F32)
    return (xf.astype(F32) + a).astype(BF16)


def capacity(t, top, n_exp):
    return ((top * ((2 * t + n_exp - 1) // n_exp) + 7) // 8) * 8


def split3(v):
    a = v.astype(BF16)
    r = v - a.astype(F32)
    b = r.astype(BF16)
    return a, b, (r - b.astype(F32)).astype(BF16)


def ranks(hit):
    t = hit.shape[-1]
    tri = (jnp.arange(t)[:, None] < jnp.arange(t)[None, :]).astype(BF16)
    n = jnp.dot(hit.reshape(-1, t).astype(BF16), tri, preferred_element_type=F32).astype(I32)
    return jnp.where(hit, n.reshape(hit.shape), NONE)


def among(idx, first, n):
    e = first + jnp.arange(n, dtype=I32)
    return idx[:, :, None, :] == e[None, None, :, None]


def expert_kernel(cap, tok, meta, pos, za, zy, zk, zm, w1, w3, w2, oa, ob, done, zb, x, act, w13b, w2b, zs, ws, os):
    el, d, f = w1.shape
    ns = pos.shape[0] // el
    t = zm.shape[0]
    z = (za, zy, zk, zm)
    fb, nb = f // LANES, d // LANES
    outs = [(oa if i < ns // 2 else ob).at[i % (ns // 2)] for i in range(ns)]

    def off(i, e):
        return pl.multiple_of(meta[i * el + e], GRAIN)

    def fetch(i):
        return pltpu.make_async_copy(z[i], zb.at[i % 2], zs.at[i % 2])

    def put(i, e):
        return pltpu.make_async_copy(x.at[e, pl.ds(off(i, e), cap)], outs[i].at[pl.ds(e * cap, cap)], os.at[i * el + e])

    def weights(e):
        s = e % 2
        cs = []
        for i in range(fb):
            for o, w in enumerate((w1, w3)):
                cs.append(pltpu.make_async_copy(w.at[e, :, pl.ds(i * LANES, LANES)],
                                                w13b.at[s, :, pl.ds((2 * i + o) * LANES, LANES)],
                                                ws.at[s, 2 * i + o]))
        cs.append(pltpu.make_async_copy(w2.at[e], w2b.at[s], ws.at[s, 2 * fb]))
        return cs

    fetch(0).start()
    fetch(1).start()
    for e in range(2):
        for c in weights(e):
            c.start()
    for i in range(ns):
        fetch(i).wait()
        row = lax.broadcasted_iota(I32, (cap, t), 0)
        sel = jnp.concatenate([jnp.where(row == pos[i * el + e:i * el + e + 1, :], 1.0, 0.0).astype(BF16) for e in range(el)], 0)
        for c in range(4):
            cols = slice(c * d // 4, (c + 1) * d // 4)
            v = jnp.dot(sel, zb[i % 2, :, cols], preferred_element_type=F32).astype(BF16)
            for e in range(el):
                x[e, pl.ds(off(i, e), cap), cols] = v[e * cap:(e + 1) * cap]
        if i + 2 < ns:
            fetch(i + 2).start()

    for e in range(el):
        s = e % 2
        for c in weights(e):
            c.wait()

        def tile(i, carry, e=e, s=s):
            rows = pl.ds(pl.multiple_of(i * TILE, TILE), TILE)
            for c in range(fb):
                h = jnp.dot(x[e, rows, :], w13b[s, :, 2 * c * LANES:2 * (c + 1) * LANES], preferred_element_type=F32)
                act[:, c * LANES:(c + 1) * LANES] = (jax.nn.silu(h[:, :LANES]) * h[:, LANES:]).astype(BF16)
            for c in range(nb // 2):
                cols = slice(2 * c * LANES, 2 * (c + 1) * LANES)
                x[e, rows, cols] = jnp.dot(act[...], w2b[s, :, cols], preferred_element_type=F32).astype(BF16)
            return carry
        lax.fori_loop(0, meta[ns * el + e], tile, 0)
        for i in range(ns):
            put(i, e).start()
        if e + 2 < el:
            for c in weights(e + 2):
                c.start()
    for e in range(el):
        for i in range(ns):
            put(i, e).wait()


def combine_kernel(cap, tok, pos, gate, ea, eb, *refs):
    *outs, done, buf, ob, es, os = refs
    ns = len(outs)
    d = outs[0].shape[1]
    n = pos.shape[0] // ns
    width = pos.shape[1]
    rows = ea.shape[1]

    def fetch(i):
        return (pltpu.make_async_copy(ea.at[i], buf.at[i % 2, pl.ds(0, rows)], es.at[i % 2, 0]),
                pltpu.make_async_copy(eb.at[i], buf.at[i % 2, pl.ds(rows, rows)], es.at[i % 2, 1]))

    def put(i):
        return pltpu.make_async_copy(ob.at[i % 2], outs[i], os.at[i % 2])

    for i in range(ns):
        for c in fetch(i):
            c.start()
    for i in range(ns):
        s = i % 2
        row = lax.broadcasted_iota(I32, (cap, width), 0)
        m = jnp.concatenate([jnp.where(row == pos[i * n + e:i * n + e + 1, :], gate[i * n + e:i * n + e + 1, :], 0.0)
                             for e in range(n)], 0)
        parts = split3(m)
        for c in fetch(i):
            c.wait()
        for c in range(4):
            cols = slice(c * d // 4, (c + 1) * d // 4)
            a = [lax.dot_general(p, buf[s, :, cols], (((0,), (0,)), ((), ())), preferred_element_type=F32) for p in parts]
            ob[s, :, cols] = a[0] + a[1] + a[2]
        put(i).start()
    for i in range(ns):
        put(i).wait()


def list_kernel(tok, pos, z, *outs):
    *outs, done = outs
    width, d = outs[0].shape
    t = z.shape[0]
    row = lax.broadcasted_iota(I32, (width, t), 0)
    for l, o in enumerate(outs):
        sel = jnp.where(row == pos[l:l + 1, :], 1.0, 0.0).astype(BF16)
        for c in range(4):
            cols = slice(c * d // 4, (c + 1) * d // 4)
            o[:, cols] = jnp.dot(sel, z[:, cols], preferred_element_type=F32).astype(BF16)


def add_kernel(tok, a, b, o, done):
    o[...] = a[...] + b[...]


def sum_kernel(tok, pos, h, *refs):
    first, second, *rest, y, done = refs
    nl = len(rest) + 1
    width, d = first.shape
    t = h.shape[0]
    lane = lax.broadcasted_iota(I32, (t, width), 1)
    hot = [jnp.where(lane == pos[:, l:l + 1], 1.0, 0.0).astype(BF16) for l in range(nl)]
    for c in range(8):
        cols = slice(c * d // 8, (c + 1) * d // 8)
        a = h[:, cols].astype(F32)
        for l in range(nl):
            v = first[:, cols] + second[:, cols] if l == 0 else rest[l - 1][:, cols]
            for p in split3(v):
                a = a + jnp.dot(hot[l], p, preferred_element_type=F32)
        y[:, cols] = a.astype(BF16)


def solution(mesh):
    ep_axes = ("row", "col")
    tok_axes = ("dp", "row", "col")
    nrow, ncol = mesh.shape["row"], mesh.shape["col"]
    ep = nrow * ncol

    def local(x, idx, gates, wq, wk, wv, wo, gattn, gmoe, w1, w3, w2):
        nm, ns, seq, d = x.shape
        t = ns * seq
        top = idx.shape[-1]
        el, _, f = w1.shape
        n_exp = el * ep
        layer = n_exp // nrow
        cap = capacity(t, top, n_exp)
        params = functools.partial(pltpu.CompilerParams, vmem_limit_bytes=67043328)
        cost = lambda n, b: pl.CostEstimate(flops=n // 100, bytes_accessed=b, transcendentals=0)
        row, col = lax.axis_index("row"), lax.axis_index("col")
        me = row * ncol + col
        chip, core = col // 2, col % 2
        tok0 = jnp.zeros((8, LANES), I32)
        token = jax.ShapeDtypeStruct((8, LANES), I32)

        pay = jnp.concatenate([idx.astype(F32), gates, jnp.zeros((nm, ns, seq, 16 - 2 * top), F32)], -1)
        pay = jnp.swapaxes(pay.reshape(nm, t, 16), 1, 2)
        every = lax.all_gather(pay, tok_axes)
        every = every.reshape((-1, ep) + every.shape[1:])

        def width_needed():
            rows_of = every[:, :, :, :top] // layer
            hit = jnp.any(rows_of[..., None] == jnp.arange(nrow, dtype=F32), axis=3)
            return jnp.max(jnp.sum(hit.astype(I32), axis=3))

        need = width_needed()
        mine = lax.dynamic_index_in_dim(every, lax.axis_index("dp"), 0, keepdims=False)

        def flip(a, axis, bit):
            return jnp.where(bit == 0, jnp.flip(a, axis), a)

        def relative(a):
            a = a.reshape((nrow, 2, 2) + a.shape[1:])
            a = jnp.flip(lax.dynamic_slice_in_dim(jnp.concatenate([a, a]), row + 1, nrow), 0)
            return flip(flip(jnp.swapaxes(a, 1, 2), 1, core), 2, chip)

        def lists_of(m):
            steps = lax.rem(row + jnp.arange(nrow, dtype=I32), nrow)
            return ranks(jnp.any(idx[m].reshape(1, t, top) // layer == steps[:, None, None], 2))

        def routes(m, width):
            ia = relative(mine[:, m, :top].astype(I32)).reshape(ep, top, t)
            ga = relative(mine[:, m, top:2 * top])[:, 1].reshape(ep // 2, top, t)
            own = lambda a: a.reshape((nrow, 2, 2) + a.shape[1:])[:, 1].reshape((ep // 2,) + a.shape[1:])
            k = 2 * el
            hits = among(ia, k * (me // 2), k)
            pos = ranks(jnp.any(hits, 1))
            g = jnp.sum(jnp.where(own(hits), ga[:, :, None, :], 0.0), 1)
            listed = ranks(jnp.any(ia // layer == row, 1))
            lists = (listed[:, :, None] == jnp.arange(width, dtype=I32)).astype(BF16)
            places = jnp.einsum("pet,ptc->pec", (jnp.maximum(pos, -1) + 1).astype(BF16), lists,
                                preferred_element_type=F32).astype(I32) - 1
            gs = jnp.einsum("pet,ptc->pec", jnp.concatenate(split3(g), 1), own(lists), preferred_element_type=F32)
            lgate = gs[:, :k] + gs[:, k:2 * k] + gs[:, 2 * k:]
            turn = lambda a: jnp.where(core == 0, a, jnp.roll(a, el, axis=1))
            places = turn(places)
            lpos = own(places).reshape(nrow, 2 * k, width)
            lgate = turn(lgate).reshape(nrow, 2 * k, width)
            cnt = turn(jnp.maximum(jnp.max(pos, -1) + 1, 0))[:, :el].reshape(nrow, 4, el)
            seg = (cnt + GRAIN - 1) // GRAIN * GRAIN
            before = jnp.arange(4)[:, None] > jnp.arange(4)[None, :]
            offs = jnp.sum(jnp.where(before[None, :, :, None], seg[:, None], 0), 2)
            tiles = (jnp.sum(seg, 1) + TILE - 1) // TILE
            meta = jnp.concatenate([offs.reshape(nrow, -1), tiles], 1)
            return places[:, :el].reshape(nrow, 4 * el, width), meta, lpos, lgate

        def send_lists(tok, pos, z, width):
            out = jax.ShapeDtypeStruct((width, d), BF16)
            *outs, tok = pl.pallas_call(
                list_kernel, out_shape=[out] * nrow + [token],
                in_specs=[ANY, VMEM, VMEM], out_specs=[VMEM] * nrow + [ANY], name="lists",
                compiler_params=params(), cost_estimate=cost(5_000_000_000, 7_000_000),
            )(tok, pos, z)
            return outs, tok

        def experts(tok, r, pos, meta, zs):
            width = pos.shape[-1]
            out = jax.ShapeDtypeStruct((2, el * cap, d), BF16)
            *outs, tok = pl.pallas_call(
                functools.partial(expert_kernel, cap), out_shape=[out, out, token],
                in_specs=[ANY, SMEM, VMEM] + [ANY] * 7, out_specs=[ANY] * 3,
                scratch_shapes=[
                    pltpu.VMEM((2, width, d), BF16),
                    pltpu.VMEM((el, -(-5 * cap // TILE) * TILE, d), BF16),
                    pltpu.VMEM((TILE, f), BF16),
                    pltpu.VMEM((2, d, 2 * f), BF16),
                    pltpu.VMEM((2, f, d), BF16),
                    pltpu.SemaphoreType.DMA((2,)),
                    pltpu.SemaphoreType.DMA((2, 2 * (f // LANES) + 1)),
                    pltpu.SemaphoreType.DMA((4 * el,)),
                ],
                compiler_params=params(), name="experts", cost_estimate=cost(35_000_000_000, 80_000_000),
            )(tok, meta[r], pos[r], *zs, w1, w3, w2)
            return outs, tok

        def combine(tok, r, lpos, lgate, ea, eb):
            width = lpos.shape[-1]
            out = jax.ShapeDtypeStruct((width, d), F32)
            *outs, tok = pl.pallas_call(
                functools.partial(combine_kernel, cap), out_shape=[out, out, token],
                in_specs=[ANY, VMEM, VMEM, ANY, ANY], out_specs=[ANY] * 3,
                scratch_shapes=[
                    pltpu.VMEM((2, 2 * el * cap, d), BF16),
                    pltpu.VMEM((2, width, d), F32),
                    pltpu.SemaphoreType.DMA((2, 2)),
                    pltpu.SemaphoreType.DMA((2,)),
                ],
                compiler_params=params(), name="combine", cost_estimate=cost(8_000_000_000, 11_000_000),
            )(tok, lpos[r], lgate[r], ea, eb)
            return outs, tok

        def add(tok, a, b):
            width = a.shape[0]
            block = pl.BlockSpec((width // 4, d), lambda i: (i, 0))
            return pl.pallas_call(
                add_kernel, grid=(4,), out_shape=[jax.ShapeDtypeStruct(a.shape, F32), token],
                in_specs=[ANY, block, block], out_specs=[block, ANY], name="add_rows",
                compiler_params=params(), cost_estimate=cost(3_000_000_000, 7_000_000),
            )(tok, a, b)

        def total(tok, home, h, parts):
            y, tok = pl.pallas_call(
                sum_kernel, out_shape=[jax.ShapeDtypeStruct((t, d), BF16), token],
                in_specs=[ANY] + [VMEM] * (2 + len(parts)), out_specs=[VMEM, ANY], name="sum_rows",
                compiler_params=params(), cost_estimate=cost(10_000_000_000, 16_000_000),
            )(tok, home, h, *parts)
            return y, tok

        def shift(r):
            return [(i, (i + r) % nrow) for i in range(nrow)]

        def layers(width, h0, z0, x):
            hs, lists = [h0], [lists_of(m) for m in range(nm)]
            rows, zy, zin = {}, {}, {}

            def spread(tok, m, z):
                out, tok = send_lists(tok, lists[m], z, width)
                for r in (0, 1, 3, 2) if m == 0 else (2, 1, 3, 0):
                    rows[str(m) + str(r)] = out[r] if r == 0 else lax.ppermute(out[r], "row", shift(r))
                return tok

            def across_chips(tok, key):
                rows[key], _ = lax.optimization_barrier((rows[key], tok))
                zy[key] = lax.ppermute(rows[key], "col", CHIP_SWAP)

            def across_cores(tok, key):
                zy[key], _ = lax.optimization_barrier((zy[key], tok))
                zin[key] = [lax.ppermute(zy[key], "col", CORE_SWAP), lax.ppermute(rows[key], "col", CORE_SWAP),
                            zy[key], rows[key]]

            blocks = [step[1:] for step in PLAN if step[0] == "X"]
            tok = spread(tok0, 0, z0)
            across_chips(tok, blocks[0])
            x1, tok = lax.optimization_barrier((x[1], tok))
            hs.append(attention(x1, wq, wk, wv, wo, gattn))
            tok = spread(tok, 1, rms(hs[1], gmoe))
            across_cores(tok, blocks[0])
            across_chips(tok, blocks[1])
            rt = [routes(m, width) for m in range(nm)]
            mineE, inE, mineP, inP, got = {}, {}, {}, {}, {}
            ys = []
            for step in PLAN:
                op, m = step[0], int(step[1])
                pos, meta, lpos, lgate = rt[m]
                key = step[1:]
                if op == "X":
                    (other, mineE[key]), tok = experts(tok, int(step[2]), pos, meta, zin[key])
                    n = blocks.index(key)
                    for k in blocks[n + 1:n + 2]:
                        across_cores(tok, k)
                    for k in blocks[n + 2:n + 3]:
                        across_chips(tok, k)
                    inE[key] = lax.ppermute(other, "col", CORE_SWAP)
                elif op == "B":
                    (other, mineP[key]), tok = combine(tok, int(step[2]), lpos, lgate, mineE[key], inE[key])
                    inP[key] = lax.ppermute(other, "col", CHIP_SWAP)
                elif op == "A":
                    s, tok = add(tok, mineP[key], inP[key])
                    got[key] = lax.ppermute(s, "row", shift(-int(step[2])))
                elif op == "W":
                    held = inP if step[2] == "0" else got
                    tok, held[key] = lax.optimization_barrier((tok, held[key]))
                else:
                    k = str(m) + "0"
                    home = jnp.pad(lists[m].T, ((0, 0), (0, LANES - nrow)))
                    y, tok = total(tok, home, hs[m], [mineP[k], inP[k]] + [got[str(m) + str(r)] for r in range(1, nrow)])
                    ys.append(y)
            return jnp.stack(ys).reshape(nm, ns, seq, d)

        h0 = attention(x[0], wq, wk, wv, wo, gattn)
        z0 = rms(h0, gmoe)
        if SINGLE:
            return layers(WIDTH, h0, z0, x)
        return lax.cond(need <= WIDTH, functools.partial(layers, WIDTH), functools.partial(layers, t), h0, z0, x)

    tok_spec = P(None, tok_axes)
    exp_spec = P(ep_axes)
    return jax.shard_map(local, mesh=mesh,
                         in_specs=(tok_spec, tok_spec, tok_spec, P(), P(), P(), P(), P(), P(), exp_spec, exp_spec, exp_spec),
                         out_specs=tok_spec, check_vma=False)
```

```python
import functools

import jax
import jax.numpy as jnp
from jax import lax
from jax.experimental import pallas as pl
from jax.experimental.pallas import tpu as pltpu
from jax.sharding import PartitionSpec as P

HEAD = 128
LANES = 128
TILE = 128
WIDTH = 288
NONE = -(1 << 20)
F32, BF16, I32 = jnp.float32, jnp.bfloat16, jnp.int32
ANY = pl.BlockSpec(memory_space=pl.ANY)
SMEM = pl.BlockSpec(memory_space=pltpu.SMEM)
VMEM = pl.BlockSpec(memory_space=pltpu.VMEM)
MESH = pl.DeviceIdType.MESH
STEPS = ((0, 1, 3, 2), (2, 3, 1, 0))


def rms(v, g):
    vf = v.astype(F32)
    return (vf * lax.rsqrt(jnp.mean(vf * vf, axis=-1, keepdims=True) + 1e-6) * g).astype(BF16)


def attention(x, wq, wk, wv, wo, g):
    ns, seq, d = x.shape
    nh = wq.shape[1] // HEAD
    xf = x.reshape(ns * seq, d)
    u = rms(xf, g)

    def proj(w):
        a = jnp.dot(u, w, preferred_element_type=F32).astype(BF16)
        return a.reshape(ns, seq, nh, HEAD)

    q, k, v = proj(wq), proj(wk), proj(wv)
    causal = jnp.arange(seq)[:, None] >= jnp.arange(seq)[None, :]
    s = jnp.einsum("bqhe,bkhe->bhqk", q, k, preferred_element_type=F32) * HEAD ** -0.5
    s = jnp.where(causal, s, -1e30)
    p = jax.nn.softmax(s, axis=-1).astype(BF16)
    o = jnp.einsum("bhqk,bkhe->bqhe", p, v, preferred_element_type=F32).astype(BF16)
    a = jnp.dot(o.reshape(ns * seq, nh * HEAD), wo, preferred_element_type=F32)
    return (xf.astype(F32) + a).astype(BF16)


def capacity(t, top, n_exp):
    return ((top * ((2 * t + n_exp - 1) // n_exp) + 7) // 8) * 8


def split3(v):
    a = v.astype(BF16)
    r = v - a.astype(F32)
    b = r.astype(BF16)
    return a, b, (r - b.astype(F32)).astype(BF16)


def ranks(hit):
    t = hit.shape[-1]
    tri = (jnp.arange(t)[:, None] < jnp.arange(t)[None, :]).astype(BF16)
    n = jnp.dot(hit.reshape(-1, t).astype(BF16), tri, preferred_element_type=F32).astype(I32)
    return jnp.where(hit, n.reshape(hit.shape), NONE)


def among(idx, first, n):
    e = first + jnp.arange(n, dtype=I32)
    return idx[:, :, None, :] == e[None, None, :, None]


def layer_kernel(cap, steps, z, h, lists, homes, px, pb, gb, w1, w3, w2,
                 y, ls, za, zy, zk, eo, em, ei, po, pm, pi, sr, rr,
                 zin, zb, x, act, w13b, w2b, ob, lsem, wsem, send, recv, ksend, krecv):
    el, d, f = w1.shape
    nm, t, _ = z.shape
    nb = steps * nm
    width = zb.shape[1]
    rows = el * cap
    fb = f // LANES
    quarter = d // 4
    dp, row, col = lax.axis_index("dp"), lax.axis_index("row"), lax.axis_index("col")
    core = (dp, row, col + 1 - 2 * lax.rem(col, 2))
    chip = (dp, row, col + 2 - 4 * (col // 2))

    def other(r):
        return (dp, lax.rem(row + r + steps, steps), col)

    def step_of(n):
        i = lax.rem(n, steps)
        i = i + (n // steps) * (steps - 1 - 2 * i)
        return lax.rem(i * (i + 1) // 2, steps)

    def remote(src, dst, kind, n, device):
        return pltpu.make_async_remote_copy(src_ref=src.at[n], dst_ref=dst.at[n], send_sem=send.at[kind, n],
                                            recv_sem=recv.at[kind, n], device_id=device, device_id_type=MESH)

    def go_row(n):
        return remote(ls, za, 0, n, other(step_of(n)))

    def go_chip(n):
        return remote(za, zy, 1, n, chip)

    def go_core(n, i):
        return pltpu.make_async_remote_copy(src_ref=(zy, za)[i].at[n], dst_ref=zk.at[n, i], send_sem=ksend.at[n, i],
                                            recv_sem=krecv.at[n, i], device_id=core, device_id_type=MESH)

    def go_expert(n):
        return remote(eo, ei, 2, n, core)

    def go_part(n):
        return remote(po, pi, 3, n, chip)

    def go_sum(n):
        return remote(sr, rr, 4, n, other(-step_of(n)))

    def local(src, dst, k):
        return pltpu.make_async_copy(src, dst, lsem.at[k])

    def run(*copies):
        for c in copies:
            c.start()
        for c in copies:
            c.wait()

    def weights(e, s):
        cs = []
        for i in range(fb):
            for o, w in enumerate((w1, w3)):
                cs.append(pltpu.make_async_copy(w.at[e, :, pl.ds(i * LANES, LANES)],
                                                w13b.at[s, :, pl.ds((2 * i + o) * LANES, LANES)],
                                                wsem.at[s, 2 * i + o]))
        cs.append(pltpu.make_async_copy(w2.at[e], w2b.at[s], wsem.at[s, 2 * fb]))
        return cs

    def hot(at, n):
        return lax.broadcasted_iota(I32, (n, at.shape[-1]), 0) == at

    barrier = pltpu.get_barrier_semaphore()
    partners = [core, chip] + [other(r) for r in range(1, steps)]
    for p in partners:
        pl.semaphore_signal(barrier, inc=1, device_id=p, device_id_type=MESH)
    for e in range(2):
        for c in weights(e, e):
            c.start()
    pl.semaphore_wait(barrier, len(partners))

    for m in range(nm):
        run(local(z.at[m], zin, 0))
        for i, r in enumerate(STEPS[m]):
            n = m * steps + i
            put = local(zb.at[i % 2], (za if r == 0 else ls).at[n], 1 + i % 2)
            sel = jnp.where(hot(lists[m, r:r + 1, :], width), 1.0, 0.0).astype(BF16)
            for c in range(4):
                cols = slice(c * quarter, (c + 1) * quarter)
                zb[i % 2, :, cols] = jnp.dot(sel, zin[:, cols], preferred_element_type=F32).astype(BF16)
            run(put)
            if r:
                go_row(n).start()
            elif m == 0:
                go_chip(n).start()

    go_row(1).wait_recv()
    go_chip(1).start()
    go_chip(0).wait_recv()
    for i in range(2):
        go_core(0, i).start()

    def dispatch(n):
        @pl.when(n + 1 < nb)
        def _():
            go_chip(n + 1).wait_recv()
            for i in range(2):
                go_core(n + 1, i).start()

        @pl.when(n + 2 < nb)
        def _():
            @pl.when(step_of(n + 2) != 0)
            def _():
                go_row(n + 2).wait_recv()
            go_chip(n + 2).start()

    def experts(n):
        for i in range(2):
            go_core(n, i).wait_recv()
        srcs = (zk.at[n, 0], zk.at[n, 1], zy.at[n], za.at[n])
        fetch = lambda i: local(srcs[i], zb.at[i % 2], 1 + i % 2)
        fetch(0).start()
        for i in range(4):
            if i + 1 < 4:
                fetch(i + 1).start()
            fetch(i).wait()
            sel = jnp.concatenate([jnp.where(hot(px[n, i * el + e:i * el + e + 1, :], cap), 1.0, 0.0).astype(BF16)
                                   for e in range(el)], 0)
            for c in range(4):
                cols = slice(c * quarter, (c + 1) * quarter)
                v = jnp.dot(sel, zb[i % 2, :, cols], preferred_element_type=F32).astype(BF16)
                for e in range(el):
                    x[e * rows + i * cap:e * rows + (i + 1) * cap, cols] = v[e * cap:(e + 1) * cap]

        def put(e, i):
            return pltpu.make_async_copy(x.at[pl.ds(pl.multiple_of(e * rows + i * cap, 32), cap)],
                                         (eo if i < 2 else em).at[n, i % 2, pl.ds(pl.multiple_of(e * cap, 32), cap)],
                                         lsem.at[3 + i])

        def expert(e, carry):
            s = lax.rem(e, 2)
            for c in weights(e, s):
                c.wait()

            def tile(k, cc):
                at = pl.ds(pl.multiple_of(e * rows + k * TILE, TILE), TILE)
                for c in range(fb):
                    v = jnp.dot(x[at, :], w13b[s, :, 2 * c * LANES:2 * (c + 1) * LANES], preferred_element_type=F32)
                    act[:, c * LANES:(c + 1) * LANES] = (jax.nn.silu(v[:, :LANES]) * v[:, LANES:]).astype(BF16)
                for c in range(d // (2 * LANES)):
                    cols = slice(2 * c * LANES, 2 * (c + 1) * LANES)
                    x[at, cols] = jnp.dot(act[...], w2b[s, :, cols], preferred_element_type=F32).astype(BF16)
                return cc
            lax.fori_loop(0, rows // TILE, tile, 0)
            run(*[put(e, i) for i in range(4)])

            @pl.when(n * el + e + 2 < nb * el)
            def _():
                for c in weights(lax.rem(e + 2, el), s):
                    c.start()
            return carry
        lax.fori_loop(0, el, expert, 0)
        go_expert(n).start()

    def combine(n):
        go_expert(n).wait_recv()
        fetch = lambda i: (local(em.at[n, i], x.at[pl.ds(2 * i * rows, rows)], 1 + 2 * i),
                           local(ei.at[n, i], x.at[pl.ds((2 * i + 1) * rows, rows)], 2 + 2 * i))
        for i in range(2):
            for c in fetch(i):
                c.start()
        k = 2 * el
        for i in range(2):
            m = jnp.concatenate([jnp.where(hot(pb[n, i * k + e:i * k + e + 1, :], cap), gb[n, i * k + e:i * k + e + 1, :], 0.0)
                                 for e in range(k)], 0)
            parts = split3(m)
            for c in fetch(i):
                c.wait()
            for c in range(4):
                cols = slice(c * quarter, (c + 1) * quarter)
                b = x[2 * i * rows:2 * (i + 1) * rows, cols]
                a = [lax.dot_general(p, b, (((0,), (0,)), ((), ())), preferred_element_type=F32) for p in parts]
                ob[i, :, cols] = a[0] + a[1] + a[2]
            put = local(ob.at[i], (po, pm)[i].at[n], 5 + i)
            put.start()
            if i == 0:
                put.wait()
                go_part(n).start()
            else:
                put.wait()

    def forward(n):
        go_part(n).wait_recv()

        @pl.when(step_of(n) != 0)
        def _():
            run(local(pm.at[n], ob.at[0], 1), local(pi.at[n], ob.at[1], 2))
            ob[0] = ob[0] + ob[1]
            run(local(ob.at[0], sr.at[n], 1))
            go_sum(n).start()

    def finish(m):
        at = [m * steps + STEPS[m].index(r) for r in range(steps)]
        for r in range(1, steps):
            go_sum(at[r]).wait_recv()
        refs = [pm.at[at[0]], pi.at[at[0]]] + [rr.at[at[r]] for r in range(1, steps)]
        lane = lax.broadcasted_iota(I32, (t, width), 1)
        fill = local(h.at[m], zin, 0)
        fill.start()
        fill.wait()
        for c in range(4):
            cols = slice(c * quarter, (c + 1) * quarter)
            spot = lambda l: ob.at[l // 4, :, pl.ds(l % 4 * quarter, quarter)]
            run(*[local(a.at[:, pl.ds(c * quarter, quarter)], spot(l), 1 + l) for l, a in enumerate(refs)])
            v = zin[:, cols].astype(F32)
            for r in range(steps):
                one = jnp.where(lane == homes[m, :, r:r + 1], 1.0, 0.0).astype(BF16)
                if r == 0:
                    u = ob[0, :, 0:quarter] + ob[0, :, quarter:2 * quarter]
                else:
                    l = r + 1
                    u = ob[l // 4, :, l % 4 * quarter:(l % 4 + 1) * quarter]
                for p in split3(u):
                    v = v + jnp.dot(one, p, preferred_element_type=F32)
            zin[:, cols] = v.astype(BF16)
        run(local(zin, y.at[m], 0))

    def block(n, carry):
        @pl.when(n < nb)
        def _():
            dispatch(n)
            experts(n)

        @pl.when(jnp.logical_and(n >= 1, n <= nb))
        def _():
            combine(n - 1)

        @pl.when(jnp.logical_and(n >= 2, n <= nb + 1))
        def _():
            forward(n - 2)

        @pl.when(n == nb - 1)
        def _():
            finish(0)

        @pl.when(n == nb + 2)
        def _():
            finish(1)
        return carry
    lax.fori_loop(0, nb + 3, block, 0)

    def drain(n, carry):
        for c in (go_chip(n), go_core(n, 0), go_core(n, 1), go_expert(n), go_part(n)):
            c.wait_send()

        @pl.when(step_of(n) != 0)
        def _():
            go_row(n).wait_send()
            go_sum(n).wait_send()
        return carry
    lax.fori_loop(0, nb, drain, 0)


def solution(mesh):
    ep_axes = ("row", "col")
    tok_axes = ("dp", "row", "col")
    nrow, ncol = mesh.shape["row"], mesh.shape["col"]
    ep = nrow * ncol

    def local(x, idx, gates, wq, wk, wv, wo, gattn, gmoe, w1, w3, w2):
        nm, ns, seq, d = x.shape
        t = ns * seq
        top = idx.shape[-1]
        el, _, f = w1.shape
        n_exp = el * ep
        layer = n_exp // nrow
        cap = capacity(t, top, n_exp)
        row, col = lax.axis_index("row"), lax.axis_index("col")
        me = row * ncol + col
        chip, core = col // 2, col % 2

        pay = jnp.concatenate([idx.astype(F32), gates, jnp.zeros((nm, ns, seq, 16 - 2 * top), F32)], -1)
        pay = jnp.swapaxes(pay.reshape(nm, t, 16), 1, 2)
        every = lax.all_gather(pay, tok_axes)
        every = every.reshape((-1, ep) + every.shape[1:])

        def width_needed():
            rows_of = every[:, :, :, :top] // layer
            hit = jnp.any(rows_of[..., None] == jnp.arange(nrow, dtype=F32), axis=3)
            return jnp.max(jnp.sum(hit.astype(I32), axis=3))

        need = width_needed()
        mine = lax.dynamic_index_in_dim(every, lax.axis_index("dp"), 0, keepdims=False)

        def flip(a, axis, bit):
            return jnp.where(bit == 0, jnp.flip(a, axis), a)

        def relative(a):
            a = a.reshape((nrow, 2, 2) + a.shape[1:])
            a = jnp.flip(lax.dynamic_slice_in_dim(jnp.concatenate([a, a]), row + 1, nrow), 0)
            return flip(flip(jnp.swapaxes(a, 1, 2), 1, core), 2, chip)

        def lists_of(m):
            steps = lax.rem(row + jnp.arange(nrow, dtype=I32), nrow)
            return ranks(jnp.any(idx[m].reshape(1, t, top) // layer == steps[:, None, None], 2))

        def routes(m, width):
            ia = relative(mine[:, m, :top].astype(I32)).reshape(ep, top, t)
            ga = relative(mine[:, m, top:2 * top])[:, 1].reshape(ep // 2, top, t)
            own = lambda a: a.reshape((nrow, 2, 2) + a.shape[1:])[:, 1].reshape((ep // 2,) + a.shape[1:])
            k = 2 * el
            hits = among(ia, k * (me // 2), k)
            pos = ranks(jnp.any(hits, 1))
            g = jnp.sum(jnp.where(own(hits), ga[:, :, None, :], 0.0), 1)
            listed = ranks(jnp.any(ia // layer == row, 1))
            lists = (listed[:, :, None] == jnp.arange(width, dtype=I32)).astype(BF16)
            places = jnp.einsum("pet,ptc->pec", (jnp.maximum(pos, -1) + 1).astype(BF16), lists,
                                preferred_element_type=F32).astype(I32) - 1
            gs = jnp.einsum("pet,ptc->pec", jnp.concatenate(split3(g), 1), own(lists), preferred_element_type=F32)
            lgate = gs[:, :k] + gs[:, k:2 * k] + gs[:, 2 * k:]
            turn = lambda a: jnp.where(core == 0, a, jnp.roll(a, el, axis=1))
            places = turn(places)
            lpos = own(places).reshape(nrow, 2 * k, width)
            lgate = turn(lgate).reshape(nrow, 2 * k, width)
            return places[:, :el].reshape(nrow, 4 * el, width), lpos, lgate

        def layers(width, zs, hs):
            lists = jnp.stack([lists_of(m) for m in range(nm)])
            homes = jnp.pad(jnp.swapaxes(lists, 1, 2), ((0, 0), (0, 0), (0, LANES - nrow)))
            rt = [routes(m, width) for m in range(nm)]
            px, pb, gb = (jnp.concatenate([jnp.stack([rt[m][k][r] for r in STEPS[m]]) for m in range(nm)]) for k in range(3))
            nb = nm * nrow
            rows = el * cap
            wide = jax.ShapeDtypeStruct((nb, width, d), BF16)
            exact = jax.ShapeDtypeStruct((nb, width, d), F32)
            pair = jax.ShapeDtypeStruct((nb, 2, rows, d), BF16)
            y, *_ = pl.pallas_call(
                functools.partial(layer_kernel, cap, nrow),
                out_shape=[jax.ShapeDtypeStruct((nm, t, d), BF16), wide, wide, wide,
                           jax.ShapeDtypeStruct((nb, 2, width, d), BF16), pair, pair, pair] + [exact] * 5,
                in_specs=[ANY] * 2 + [VMEM] * 5 + [ANY] * 3, out_specs=[ANY] * 13,
                scratch_shapes=[
                    pltpu.VMEM((t, d), BF16),
                    pltpu.VMEM((2, width, d), BF16),
                    pltpu.VMEM((4 * rows, d), BF16),
                    pltpu.VMEM((TILE, f), BF16),
                    pltpu.VMEM((2, d, 2 * f), BF16),
                    pltpu.VMEM((2, f, d), BF16),
                    pltpu.VMEM((2, width, d), F32),
                    pltpu.SemaphoreType.DMA((8,)),
                    pltpu.SemaphoreType.DMA((2, 2 * (f // LANES) + 1)),
                    pltpu.SemaphoreType.DMA((5, nb)),
                    pltpu.SemaphoreType.DMA((5, nb)),
                    pltpu.SemaphoreType.DMA((nb, 2)),
                    pltpu.SemaphoreType.DMA((nb, 2)),
                ],
                compiler_params=pltpu.CompilerParams(vmem_limit_bytes=67043328, has_side_effects=True,
                                                     collective_id=0 if width < t else 1),
                name="layer",
            )(zs, hs, lists, homes, px, pb, gb, w1, w3, w2)
            return y.reshape(nm, ns, seq, d)

        hs = jnp.stack([attention(x[m], wq, wk, wv, wo, gattn) for m in range(nm)])
        zs = rms(hs, gmoe)
        return lax.cond(need <= WIDTH, functools.partial(layers, WIDTH), functools.partial(layers, t), zs, hs)

    tok_spec = P(None, tok_axes)
    exp_spec = P(ep_axes)
    return jax.shard_map(local, mesh=mesh,
                         in_specs=(tok_spec, tok_spec, tok_spec, P(), P(), P(), P(), P(), P(), exp_spec, exp_spec, exp_spec),
                         out_specs=tok_spec, check_vma=False)
```

```python
import functools

import jax
import jax.numpy as jnp
from jax import lax
from jax.experimental import pallas as pl
from jax.experimental.pallas import tpu as pltpu
from jax.sharding import PartitionSpec as P

HEAD = 128
LANES = 128
TILE = 128
WIDTH, WINDOW = 288, 208
NONE = -(1 << 20)
F32, BF16, I32 = jnp.float32, jnp.bfloat16, jnp.int32
ANY = pl.BlockSpec(memory_space=pl.ANY)
SMEM = pl.BlockSpec(memory_space=pltpu.SMEM)
VMEM = pl.BlockSpec(memory_space=pltpu.VMEM)
MESH = pl.DeviceIdType.MESH
STEPS = ((0, 1, 3, 2), (2, 3, 1, 0))


def rms(v, g):
    vf = v.astype(F32)
    return (vf * lax.rsqrt(jnp.mean(vf * vf, axis=-1, keepdims=True) + 1e-6) * g).astype(BF16)


def attention(x, wq, wk, wv, wo, g):
    ns, seq, d = x.shape
    nh = wq.shape[1] // HEAD
    xf = x.reshape(ns * seq, d)
    u = rms(xf, g)

    def proj(w):
        a = jnp.dot(u, w, preferred_element_type=F32).astype(BF16)
        return a.reshape(ns, seq, nh, HEAD)

    q, k, v = proj(wq), proj(wk), proj(wv)
    causal = jnp.arange(seq)[:, None] >= jnp.arange(seq)[None, :]
    s = jnp.einsum("bqhe,bkhe->bhqk", q, k, preferred_element_type=F32) * HEAD ** -0.5
    s = jnp.where(causal, s, -1e30)
    p = jax.nn.softmax(s, axis=-1).astype(BF16)
    o = jnp.einsum("bhqk,bkhe->bqhe", p, v, preferred_element_type=F32).astype(BF16)
    a = jnp.dot(o.reshape(ns * seq, nh * HEAD), wo, preferred_element_type=F32)
    return (xf.astype(F32) + a).astype(BF16)


def capacity(t, top, n_exp):
    return ((top * ((2 * t + n_exp - 1) // n_exp) + 7) // 8) * 8


def split3(v):
    a = v.astype(BF16)
    r = v - a.astype(F32)
    b = r.astype(BF16)
    return a, b, (r - b.astype(F32)).astype(BF16)


def ranks(hit):
    t = hit.shape[-1]
    tri = (jnp.arange(t)[:, None] < jnp.arange(t)[None, :]).astype(BF16)
    n = jnp.dot(hit.reshape(-1, t).astype(BF16), tri, preferred_element_type=F32).astype(I32)
    return jnp.where(hit, n.reshape(hit.shape), NONE)


def among(idx, first, n):
    e = first + jnp.arange(n, dtype=I32)
    return idx[:, :, None, :] == e[None, None, :, None]


def list_kernel(pos, z, *outs):
    width, d = outs[0].shape
    row = lax.broadcasted_iota(I32, (width, z.shape[0]), 0)
    for l, o in enumerate(outs):
        sel = jnp.where(row == pos[l:l + 1, :], 1.0, 0.0).astype(BF16)
        for c in range(4):
            cols = slice(c * d // 4, (c + 1) * d // 4)
            o[:, cols] = jnp.dot(sel, z[:, cols], preferred_element_type=F32).astype(BF16)


def layer_kernel(cap, steps, z0, z1, h0, h1, lists, homes, px, pb, gb, w1, w3, w2,
                 y, ls, z2, zy, zk, eo, em, ei, po, pm, pi, sr, rr,
                 zin, zb, x, act, w13b, w2b, ob, lsem, psem, wsem, send, recv, ksend, krecv):
    el, d, f = w1.shape
    t, _ = z1.shape
    h = (h0, h1)
    nm = len(h)
    nb = steps * nm
    width, window = zb.shape[1], zy.shape[1]
    gap = width - window
    rows = el * cap
    fb = f // LANES
    quarter = d // 4
    dp, row, col = lax.axis_index("dp"), lax.axis_index("row"), lax.axis_index("col")
    near = pl.ds(pl.multiple_of(gap * (col // 2), 16), window)
    far = pl.ds(pl.multiple_of(gap * (1 - col // 2), 16), window)
    core = (dp, row, col + 1 - 2 * lax.rem(col, 2))
    chip = (dp, row, col + 2 - 4 * (col // 2))

    def other(r):
        return (dp, lax.rem(row + r + steps, steps), col)

    def step_of(n):
        i = lax.rem(n, steps)
        i = i + (n // steps) * (steps - 1 - 2 * i)
        return lax.rem(i * (i + 1) // 2, steps)

    def remote(src, dst, kind, n, device):
        return pltpu.make_async_remote_copy(src_ref=src.at[n], dst_ref=dst.at[n], send_sem=send.at[kind, n],
                                            recv_sem=recv.at[kind, n], device_id=device, device_id_type=MESH)

    def pair(src, dst, send_sem, recv_sem, device):
        return pltpu.make_async_remote_copy(src_ref=src, dst_ref=dst, send_sem=send_sem, recv_sem=recv_sem,
                                            device_id=device, device_id_type=MESH)

    def by_half(n, act_on):
        if isinstance(n, int):
            act_on(z0.at[n] if n < steps else z2.at[n - steps])
            return

        @pl.when(n < steps)
        def _():
            act_on(z0.at[n])

        @pl.when(n >= steps)
        def _():
            act_on(z2.at[n - steps])

    def go_row(n):
        return pair(ls.at[n - steps], z2.at[n - steps], send.at[0, n], recv.at[0, n], other(step_of(n)))

    def go_chip(n, src=None):
        src = z0.at[0] if src is None else src
        return pair(src.at[far], zy.at[n], send.at[1, n], recv.at[1, n], chip)

    def start_chip(n):
        by_half(n, lambda src: go_chip(n, src).start())

    def go_core(n, i, src=None):
        src = zy.at[n] if i == 0 else (z0.at[0] if src is None else src).at[near]
        return pair(src, zk.at[n, i], ksend.at[n, i], krecv.at[n, i], core)

    def start_core(n):
        go_core(n, 0).start()
        by_half(n, lambda src: go_core(n, 1, src).start())

    def go_expert(n):
        return remote(eo, ei, 2, n, core)

    def go_part(n):
        return remote(po, pi, 3, n, chip)

    def go_sum(n):
        return remote(sr, rr, 4, n, other(-step_of(n)))

    def local(src, dst, k):
        return pltpu.make_async_copy(src, dst, lsem.at[k])

    def run(*copies):
        for c in copies:
            c.start()
        for c in copies:
            c.wait()

    def weights(e, s):
        cs = []
        for i in range(fb):
            for o, w in enumerate((w1, w3)):
                cs.append(pltpu.make_async_copy(w.at[e, :, pl.ds(i * LANES, LANES)],
                                                w13b.at[s, :, pl.ds((2 * i + o) * LANES, LANES)],
                                                wsem.at[s, 2 * i + o]))
        cs.append(pltpu.make_async_copy(w2.at[e], w2b.at[s], wsem.at[s, 2 * fb]))
        return cs

    def hot(at, n):
        return lax.broadcasted_iota(I32, (n, at.shape[-1]), 0) == at

    barrier = pltpu.get_barrier_semaphore()
    partners = [core, chip] + [other(r) for r in range(1, steps)]
    for p in partners:
        pl.semaphore_signal(barrier, inc=1, device_id=p, device_id_type=MESH)
    for e in range(2):
        for c in weights(e, e):
            c.start()
    pl.semaphore_wait(barrier, len(partners))

    start_chip(0)
    run(local(z1, zin, 0))
    for i, r in enumerate(STEPS[1]):
        n = steps + i
        put = local(zb.at[i % 2], (z2 if r == 0 else ls).at[i], 1 + i % 2)
        sel = jnp.where(hot(lists[r:r + 1, :], width), 1.0, 0.0).astype(BF16)
        for c in range(4):
            cols = slice(c * quarter, (c + 1) * quarter)
            zb[i % 2, :, cols] = jnp.dot(sel, zin[:, cols], preferred_element_type=F32).astype(BF16)
        run(put)
        if r:
            go_row(n).start()
        if i == 0:
            go_chip(0).wait_recv()
            start_core(0)
            start_chip(1)

    def dispatch(n):
        @pl.when(n + 1 < nb)
        def _():
            go_chip(n + 1).wait_recv()
            start_core(n + 1)

        @pl.when(n + 2 < nb)
        def _():
            @pl.when(jnp.logical_and(n + 2 >= steps, step_of(n + 2) != 0))
            def _():
                go_row(n + 2).wait_recv()
            start_chip(n + 2)

    def experts(n):
        for i in range(2):
            go_core(n, i).wait_recv()
        srcs = (zk.at[n, 0], zk.at[n, 1], zy.at[n])
        fetch = lambda i, src: local(src, zb.at[i % 2, pl.ds(0, window)], 1 + i % 2)
        fetch(0, srcs[0]).start()
        for i in range(4):
            if i + 1 < 3:
                fetch(i + 1, srcs[i + 1]).start()
            elif i + 1 == 3:
                by_half(n, lambda src: fetch(3, src.at[near]).start())
            fetch(i, srcs[min(i, 2)]).wait()
            sel = jnp.concatenate([jnp.where(hot(px[n, i * el + e:i * el + e + 1, :], cap), 1.0, 0.0).astype(BF16)
                                   for e in range(el)], 0)
            for c in range(4):
                cols = slice(c * quarter, (c + 1) * quarter)
                v = jnp.dot(sel, zb[i % 2, 0:window, cols], preferred_element_type=F32).astype(BF16)
                for e in range(el):
                    x[e * rows + i * cap:e * rows + (i + 1) * cap, cols] = v[e * cap:(e + 1) * cap]

        def put(e, i):
            return pltpu.make_async_copy(x.at[pl.ds(pl.multiple_of(e * rows + i * cap, 32), cap)],
                                         (eo if i < 2 else em).at[n, i % 2, pl.ds(pl.multiple_of(e * cap, 32), cap)],
                                         psem.at[e, i])

        def expert(e, carry):
            s = lax.rem(e, 2)
            for c in weights(e, s):
                c.wait()

            def tile(k, cc):
                at = pl.ds(pl.multiple_of(e * rows + k * TILE, TILE), TILE)
                for c in range(fb):
                    v = jnp.dot(x[at, :], w13b[s, :, 2 * c * LANES:2 * (c + 1) * LANES], preferred_element_type=F32)
                    act[:, c * LANES:(c + 1) * LANES] = (jax.nn.silu(v[:, :LANES]) * v[:, LANES:]).astype(BF16)
                for c in range(d // (2 * LANES)):
                    cols = slice(2 * c * LANES, 2 * (c + 1) * LANES)
                    x[at, cols] = jnp.dot(act[...], w2b[s, :, cols], preferred_element_type=F32).astype(BF16)
                return cc
            lax.fori_loop(0, rows // TILE, tile, 0)
            for i in range(4):
                put(e, i).start()

            @pl.when(n * el + e + 2 < nb * el)
            def _():
                for c in weights(lax.rem(e + 2, el), s):
                    c.start()
            return carry
        lax.fori_loop(0, el, expert, 0)
        for e in range(el):
            for i in range(4):
                put(e, i).wait()
        go_expert(n).start()

    def combine(n):
        go_expert(n).wait_recv()
        fetch = lambda i: (local(em.at[n, i], x.at[pl.ds(2 * i * rows, rows)], 1 + 2 * i),
                           local(ei.at[n, i], x.at[pl.ds((2 * i + 1) * rows, rows)], 2 + 2 * i))
        for i in range(2):
            for c in fetch(i):
                c.start()
        k = 2 * el
        for i in range(2):
            m = jnp.concatenate([jnp.where(hot(pb[n, i * k + e:i * k + e + 1, :], cap), gb[n, i * k + e:i * k + e + 1, :], 0.0)
                                 for e in range(k)], 0)
            parts = split3(m)
            for c in fetch(i):
                c.wait()
            for c in range(4):
                cols = slice(c * quarter, (c + 1) * quarter)
                b = x[2 * i * rows:2 * (i + 1) * rows, cols]
                a = [lax.dot_general(p, b, (((0,), (0,)), ((), ())), preferred_element_type=F32) for p in parts]
                ob[i, 0:window, cols] = a[0] + a[1] + a[2]
            put = local(ob.at[i, pl.ds(0, window)], (po, pm)[i].at[n], 5 + i)
            put.start()
            if i == 0:
                put.wait()
                go_part(n).start()
            else:
                put.wait()

    def forward(n):
        go_part(n).wait_recv()

        copies = (local(pm.at[n], ob.at[0, near], 1), local(pi.at[n], ob.at[1, far], 2))
        for c in copies:
            c.start()
        if gap:
            for i, first in enumerate((1 - col // 2, col // 2)):
                ob[i, pl.ds(pl.multiple_of(window * first, 16), gap), :] = jnp.zeros((gap, d), F32)
        for c in copies:
            c.wait()
        ob[0] = ob[0] + ob[1]
        run(local(ob.at[0], sr.at[n], 1))

        @pl.when(step_of(n) != 0)
        def _():
            go_sum(n).start()

    def finish(m):
        at = [m * steps + STEPS[m].index(r) for r in range(steps)]
        for r in range(1, steps):
            go_sum(at[r]).wait_recv()
        refs = [sr.at[at[0]]] + [rr.at[at[r]] for r in range(1, steps)]
        lane = lax.broadcasted_iota(I32, (t, width), 1)
        run(local(h[m], zin, 0))
        for c in range(4):
            cols = slice(c * quarter, (c + 1) * quarter)
            spot = lambda l: ob.at[0, :, pl.ds(l * quarter, quarter)]
            run(*[local(a.at[:, pl.ds(c * quarter, quarter)], spot(l), 1 + l) for l, a in enumerate(refs)])
            v = zin[:, cols].astype(F32)
            for r in range(steps):
                one = jnp.where(lane == homes[m, :, r:r + 1], 1.0, 0.0).astype(BF16)
                for p in split3(ob[0, :, r * quarter:(r + 1) * quarter]):
                    v = v + jnp.dot(one, p, preferred_element_type=F32)
            zin[:, cols] = v.astype(BF16)
        run(local(zin, y.at[m], 0))

    def block(n, carry):
        @pl.when(n < nb)
        def _():
            dispatch(n)
            experts(n)

        @pl.when(jnp.logical_and(n >= 1, n <= nb))
        def _():
            combine(n - 1)

        @pl.when(jnp.logical_and(n >= 2, n <= nb + 1))
        def _():
            forward(n - 2)

        @pl.when(n == nb - 1)
        def _():
            finish(0)

        @pl.when(n == nb + 2)
        def _():
            finish(1)
        return carry
    lax.fori_loop(0, nb + 3, block, 0)

    def drain(n, carry):
        for c in (go_chip(n), go_core(n, 0), go_core(n, 1), go_expert(n), go_part(n)):
            c.wait_send()

        @pl.when(step_of(n) != 0)
        def _():
            go_sum(n).wait_send()

            @pl.when(n >= steps)
            def _():
                go_row(n).wait_send()
        return carry
    lax.fori_loop(0, nb, drain, 0)


def solution(mesh):
    ep_axes = ("row", "col")
    tok_axes = ("dp", "row", "col")
    nrow, ncol = mesh.shape["row"], mesh.shape["col"]
    ep = nrow * ncol

    def local(x, idx, gates, wq, wk, wv, wo, gattn, gmoe, w1, w3, w2):
        nm, ns, seq, d = x.shape
        t = ns * seq
        top = idx.shape[-1]
        el, _, f = w1.shape
        n_exp = el * ep
        layer = n_exp // nrow
        cap = capacity(t, top, n_exp)
        row, col = lax.axis_index("row"), lax.axis_index("col")
        me = row * ncol + col
        chip, core = col // 2, col % 2

        pay = jnp.concatenate([idx.astype(F32), gates, jnp.zeros((nm, ns, seq, 16 - 2 * top), F32)], -1)
        pay = jnp.swapaxes(pay.reshape(nm, t, 16), 1, 2)
        every = lax.all_gather(pay, tok_axes)
        every = every.reshape((-1, ep) + every.shape[1:])

        def halves(idx_, first):
            half = layer // 2
            return [jnp.any(idx_ // half == 2 * first + c, -2) for c in range(2)]

        def width_needed(gap):
            need = 0
            for r in range(nrow):
                a, b = halves(every[:, :, :, :top].astype(I32), r)
                na, nb, both = (jnp.sum(v.astype(I32), -1) for v in (a & ~b, b & ~a, a & b))
                need = jnp.maximum(need, jnp.max(jnp.maximum(na, gap) + both + jnp.maximum(nb, gap)))
            return need

        def places_of(a, b, gap, width):
            only = [ranks(v) for v in (a & ~b, a & b, b & ~a)]
            na = jnp.sum((a & ~b).astype(I32), -1, keepdims=True)
            mid = jnp.maximum(na, gap)
            return jnp.where(a & b, mid + only[1], jnp.where(a, only[0], jnp.where(b, width - 1 - only[2], NONE)))

        mine = lax.dynamic_index_in_dim(every, lax.axis_index("dp"), 0, keepdims=False)

        def flip(a, axis, bit):
            return jnp.where(bit == 0, jnp.flip(a, axis), a)

        def relative(a):
            a = a.reshape((nrow, 2, 2) + a.shape[1:])
            a = jnp.flip(lax.dynamic_slice_in_dim(jnp.concatenate([a, a]), row + 1, nrow), 0)
            return flip(flip(jnp.swapaxes(a, 1, 2), 1, core), 2, chip)

        def lists_of(m, width, window):
            steps = lax.rem(row + jnp.arange(nrow, dtype=I32), nrow)
            own = jnp.broadcast_to(idx[m].reshape(t, top).T[None], (nrow, top, t))
            return places_of(*halves(own, steps[:, None, None]), width - window, width)

        def routes(m, width, window):
            ia = relative(mine[:, m, :top].astype(I32)).reshape(ep, top, t)
            ga = relative(mine[:, m, top:2 * top])[:, 1].reshape(ep // 2, top, t)
            own = lambda a: a.reshape((nrow, 2, 2) + a.shape[1:])[:, 1].reshape((ep // 2,) + a.shape[1:])
            k = 2 * el
            hits = among(ia, k * (me // 2), k)
            pos = ranks(jnp.any(hits, 1))
            g = jnp.sum(jnp.where(own(hits), ga[:, :, None, :], 0.0), 1)
            listed = places_of(*halves(ia, row), width - window, width) - chip * (width - window)
            lists = (listed[:, :, None] == jnp.arange(window, dtype=I32)).astype(BF16)
            places = jnp.einsum("pet,ptc->pec", (jnp.maximum(pos, -1) + 1).astype(BF16), lists,
                                preferred_element_type=F32).astype(I32) - 1
            gs = jnp.einsum("pet,ptc->pec", jnp.concatenate(split3(g), 1), own(lists), preferred_element_type=F32)
            lgate = gs[:, :k] + gs[:, k:2 * k] + gs[:, 2 * k:]
            turn = lambda a: jnp.where(core == 0, a, jnp.roll(a, el, axis=1))
            places = turn(places)
            lpos = own(places).reshape(nrow, 2 * k, window)
            lgate = turn(lgate).reshape(nrow, 2 * k, window)
            return places[:, :el].reshape(nrow, 4 * el, window), lpos, lgate

        def layers(width, window, z0, h0, x):
            lists = [lists_of(m, width, window) for m in range(nm)]
            out = jax.ShapeDtypeStruct((width, d), BF16)
            rows0 = pl.pallas_call(
                list_kernel, out_shape=[out] * nrow, in_specs=[VMEM, VMEM], out_specs=[VMEM] * nrow, name="lists",
                compiler_params=pltpu.CompilerParams(vmem_limit_bytes=67043328),
                cost_estimate=pl.CostEstimate(flops=50_000_000, bytes_accessed=7_000_000, transcendentals=0),
            )(lists[0], z0)
            came = jnp.stack([rows0[r] if r == 0 else lax.ppermute(rows0[r], "row", [(i, (i + r) % nrow) for i in range(nrow)])
                              for r in STEPS[0]])
            x1, _ = lax.optimization_barrier((x[1], rows0[0]))
            h1 = attention(x1, wq, wk, wv, wo, gattn)
            z1 = rms(h1, gmoe)
            homes = jnp.stack([jnp.pad(a.T, ((0, 0), (0, LANES - nrow))) for a in lists])
            rt = [routes(m, width, window) for m in range(nm)]
            px, pb, gb = (jnp.concatenate([jnp.stack([rt[m][k][r] for r in STEPS[m]]) for m in range(nm)]) for k in range(3))
            nb = nm * nrow
            rows = el * cap
            wide = jax.ShapeDtypeStruct((nrow, width, d), BF16)
            part = jax.ShapeDtypeStruct((nb, window, d), F32)
            exact = jax.ShapeDtypeStruct((nb, width, d), F32)
            pair = jax.ShapeDtypeStruct((nb, 2, rows, d), BF16)
            y, *_ = pl.pallas_call(
                functools.partial(layer_kernel, cap, nrow),
                out_shape=[jax.ShapeDtypeStruct((nm, t, d), BF16), wide, wide, jax.ShapeDtypeStruct((nb, window, d), BF16),
                           jax.ShapeDtypeStruct((nb, 2, window, d), BF16), pair, pair, pair] + [part] * 3 + [exact] * 2,
                in_specs=[ANY] * 4 + [VMEM] * 5 + [ANY] * 3, out_specs=[ANY] * 13,
                scratch_shapes=[
                    pltpu.VMEM((t, d), BF16),
                    pltpu.VMEM((2, width, d), BF16),
                    pltpu.VMEM((4 * rows, d), BF16),
                    pltpu.VMEM((TILE, f), BF16),
                    pltpu.VMEM((2, d, 2 * f), BF16),
                    pltpu.VMEM((2, f, d), BF16),
                    pltpu.VMEM((2, width, d), F32),
                    pltpu.SemaphoreType.DMA((8,)),
                    pltpu.SemaphoreType.DMA((el, 4)),
                    pltpu.SemaphoreType.DMA((2, 2 * (f // LANES) + 1)),
                    pltpu.SemaphoreType.DMA((5, nb)),
                    pltpu.SemaphoreType.DMA((5, nb)),
                    pltpu.SemaphoreType.DMA((nb, 2)),
                    pltpu.SemaphoreType.DMA((nb, 2)),
                ],
                compiler_params=pltpu.CompilerParams(vmem_limit_bytes=67043328, has_side_effects=True,
                                                     collective_id=0 if width < t else 1),
                name="layer",
            )(came, z1, h0, h1, lists[1], homes, px, pb, gb, w1, w3, w2)
            return y.reshape(nm, ns, seq, d)

        h0 = attention(x[0], wq, wk, wv, wo, gattn)
        z0 = rms(h0, gmoe)
        fits = width_needed(WIDTH - WINDOW) <= WIDTH
        return lax.cond(fits, functools.partial(layers, WIDTH, WINDOW), functools.partial(layers, t, t), z0, h0, x)

    tok_spec = P(None, tok_axes)
    exp_spec = P(ep_axes)
    return jax.shard_map(local, mesh=mesh,
                         in_specs=(tok_spec, tok_spec, tok_spec, P(), P(), P(), P(), P(), P(), exp_spec, exp_spec, exp_spec),
                         out_specs=tok_spec, check_vma=False)
```

```python
import functools

import jax
import jax.numpy as jnp
from jax import lax
from jax.experimental import pallas as pl
from jax.experimental.pallas import tpu as pltpu
from jax.sharding import PartitionSpec as P

HEAD = 128
LANES = 128
TILE = 384
WIDTH, WINDOW = 288, 208
NONE = -(1 << 20)
F32, BF16, I32 = jnp.float32, jnp.bfloat16, jnp.int32
ANY = pl.BlockSpec(memory_space=pl.ANY)
SMEM = pl.BlockSpec(memory_space=pltpu.SMEM)
VMEM = pl.BlockSpec(memory_space=pltpu.VMEM)
MESH = pl.DeviceIdType.MESH
STEPS = ((0, 1, 3, 2), (2, 3, 1, 0))


def rms(v, g):
    vf = v.astype(F32)
    return (vf * lax.rsqrt(jnp.mean(vf * vf, axis=-1, keepdims=True) + 1e-6) * g).astype(BF16)


def attention_kernel(x, ga, gm, wq, wk, wv, wo, h, z, u, acc):
    i = pl.program_id(0)
    t = x.shape[0]
    half = t // 2

    @pl.when(i == 0)
    def _():
        for c in range(4):
            rows = slice(c * t // 4, (c + 1) * t // 4)
            u[rows] = rms(x[rows], ga[...])
        acc[...] = jnp.zeros_like(acc)

    q, k, v = (jnp.dot(u[...], w[...], preferred_element_type=F32).astype(BF16) for w in (wq, wk, wv))
    heads = []
    for e in range(q.shape[1] // HEAD):
        cols = slice(e * HEAD, (e + 1) * HEAD)
        parts = []
        for b in range(2):
            keys = (b + 1) * half
            w = lax.dot_general(q[b * half:(b + 1) * half, cols], k[:keys, cols], (((1,), (1,)), ((), ())),
                                preferred_element_type=F32) * HEAD ** -0.5
            seen = (lax.broadcasted_iota(I32, (half, keys), 0) + b * half) >= lax.broadcasted_iota(I32, (half, keys), 1)
            w = jnp.where(seen, w, -1e30)
            p = jnp.exp(w - jnp.max(w, axis=1, keepdims=True))
            p = (p * (1.0 / jnp.sum(p, axis=1, keepdims=True))).astype(BF16)
            parts.append(jnp.dot(p, v[:keys, cols], preferred_element_type=F32).astype(BF16))
        heads.append(jnp.concatenate(parts, 0))
    acc[...] += jnp.dot(jnp.concatenate(heads, 1), wo[...], preferred_element_type=F32)

    @pl.when(i == pl.num_programs(0) - 1)
    def _():
        for c in range(4):
            rows = slice(c * t // 4, (c + 1) * t // 4)
            r = (x[rows].astype(F32) + acc[rows]).astype(BF16)
            h[rows] = r
            z[rows] = rms(r, gm[...])


def attention(x, ga, gm, wq, wk, wv, wo):
    t, d = x.shape
    step = 2 * HEAD
    whole = pl.BlockSpec((t, d), lambda i: (0, 0))
    gain = pl.BlockSpec((1, d), lambda i: (0, 0))
    down = pl.BlockSpec((d, step), lambda i: (0, i))
    out = jax.ShapeDtypeStruct((t, d), BF16)
    return pl.pallas_call(
        attention_kernel, grid=(wq.shape[1] // step,), out_shape=[out, out],
        in_specs=[whole, gain, gain, down, down, down, pl.BlockSpec((step, d), lambda i: (i, 0))],
        out_specs=[whole, whole], scratch_shapes=[pltpu.VMEM((t, d), BF16), pltpu.VMEM((t, d), F32)],
        compiler_params=pltpu.CompilerParams(vmem_limit_bytes=67043328), name="attention",
        cost_estimate=pl.CostEstimate(flops=200_000_000, bytes_accessed=40_000_000, transcendentals=0),
    )(x, ga[None], gm[None], wq, wk, wv, wo)


def capacity(t, top, n_exp):
    return ((top * ((2 * t + n_exp - 1) // n_exp) + 7) // 8) * 8


def split3(v):
    a = v.astype(BF16)
    r = v - a.astype(F32)
    b = r.astype(BF16)
    return a, b, (r - b.astype(F32)).astype(BF16)


def ranks(hit):
    t = hit.shape[-1]
    tri = (jnp.arange(t)[:, None] < jnp.arange(t)[None, :]).astype(BF16)
    n = jnp.dot(hit.reshape(-1, t).astype(BF16), tri, preferred_element_type=F32).astype(I32)
    return jnp.where(hit, n.reshape(hit.shape), NONE)


def among(idx, first, n):
    e = first + jnp.arange(n, dtype=I32)
    return idx[:, :, None, :] == e[None, None, :, None]


def routes_kernel(top, el, gap, spot, pay, px, pb, gb, tri):
    nm, ep, _, t = pay.shape
    nb, _, window = px.shape
    steps = nb // nm
    row, chip, core = spot[0], spot[1], spot[2]
    tri[...] = jnp.where(lax.broadcasted_iota(I32, (t, t), 0) < lax.broadcasted_iota(I32, (t, t), 1), 1.0, 0.0).astype(BF16)
    per = 2 * el
    first = (row * 2 + chip) * per
    e = lax.broadcasted_iota(I32, (per, 1), 0)
    mine = (first + lax.rem(e + el * core, per)).astype(F32)
    edge = (row * 2 * per).astype(F32)
    for n in range(nb):
        m, r = n // steps, STEPS[n // steps][n % steps]

        def source(i, carry):
            far_core, far_chip = 1 - i // 2, 1 - lax.rem(i, 2)
            k = core + far_core - 2 * core * far_core
            y = chip + far_chip - 2 * chip * far_chip
            p = lax.rem(row - r + steps, steps) * 4 + y * 2 + k
            chosen = pay[m, p, 0:top, :]
            gate = pay[m, p, top:2 * top, :]
            hit = jnp.zeros((per, t), F32)
            g = jnp.zeros((per, t), F32)
            in_a = jnp.zeros((1, t), F32)
            in_b = jnp.zeros((1, t), F32)
            for j in range(top):
                c = chosen[j:j + 1, :]
                same = c == mine
                hit = hit + jnp.where(same, 1.0, 0.0)
                g = g + jnp.where(same, gate[j:j + 1, :], 0.0)
                in_a = jnp.maximum(in_a, jnp.where((c >= edge) & (c < edge + per), 1.0, 0.0))
                in_b = jnp.maximum(in_b, jnp.where((c >= edge + per) & (c < edge + 2 * per), 1.0, 0.0))
            both = in_a * in_b
            kinds = jnp.concatenate([in_a - both, both, in_b - both, jnp.zeros((5, t), F32)], 0)
            rank = jnp.dot(jnp.concatenate([hit, kinds], 0).astype(BF16), tri[...], preferred_element_type=F32)
            na = jnp.sum(in_a - both, axis=1, keepdims=True)
            place = jnp.where(both > 0, jnp.maximum(na, float(gap)) + rank[per + 1:per + 2],
                              jnp.where(in_a > 0, rank[per:per + 1],
                                        jnp.where(in_b > 0, window + gap - 1.0 - rank[per + 2:per + 3], float(NONE))))
            place = (place - (chip * gap).astype(F32)).astype(I32)
            one = jnp.where(lax.broadcasted_iota(I32, (window, t), 0) == place, 1.0, 0.0).astype(BF16)
            wanted = jnp.where(hit > 0, rank[0:per] + 1.0, 0.0).astype(BF16)
            cols = jnp.concatenate([wanted.astype(F32)] + [v.astype(F32) for v in split3(g)], 0).astype(BF16)
            rows = lax.dot_general(cols, one, (((1,), (1,)), ((), ())), preferred_element_type=F32)
            at = rows[0:per].astype(I32) - 1
            px[n, pl.ds(i * el, el), :] = at[0:el]

            @pl.when(i >= 2)
            def _():
                pb[n, pl.ds((i - 2) * per, per), :] = at
                gb[n, pl.ds((i - 2) * per, per), :] = rows[per:2 * per] + rows[2 * per:3 * per] + rows[3 * per:]
            return carry
        for i in range(4):
            source(i, 0)


def list_kernel(pos, z, *outs):
    width, d = outs[0].shape
    row = lax.broadcasted_iota(I32, (width, z.shape[0]), 0)
    for l, o in enumerate(outs):
        sel = jnp.where(row == pos[l:l + 1, :], 1.0, 0.0).astype(BF16)
        for c in range(4):
            cols = slice(c * d // 4, (c + 1) * d // 4)
            o[:, cols] = jnp.dot(sel, z[:, cols], preferred_element_type=F32).astype(BF16)


def layer_kernel(cap, steps, z0, z1, h0, h1, lists, homes, px, pb, gb, w1, w3, w2,
                 y, ls, z2, zy, zk, eo, em, ei, po, pm, pi, sr, rr,
                 zin, zb, x, act, w13b, w2b, ob, lsem, psem, wsem, send, recv, ksend, krecv):
    el, d, f = w1.shape
    t, _ = z1.shape
    h = (h0, h1)
    nm = len(h)
    nb = steps * nm
    width, window = zb.shape[1], zy.shape[1]
    gap = width - window
    rows = el * cap
    fb = f // LANES
    quarter = d // 4
    dp, row, col = lax.axis_index("dp"), lax.axis_index("row"), lax.axis_index("col")
    near = pl.ds(pl.multiple_of(gap * (col // 2), 16), window)
    far = pl.ds(pl.multiple_of(gap * (1 - col // 2), 16), window)
    core = (dp, row, col + 1 - 2 * lax.rem(col, 2))
    chip = (dp, row, col + 2 - 4 * (col // 2))

    def other(r):
        return (dp, lax.rem(row + r + steps, steps), col)

    def step_of(n):
        i = lax.rem(n, steps)
        i = i + (n // steps) * (steps - 1 - 2 * i)
        return lax.rem(i * (i + 1) // 2, steps)

    def remote(src, dst, kind, n, device):
        return pltpu.make_async_remote_copy(src_ref=src.at[n], dst_ref=dst.at[n], send_sem=send.at[kind, n],
                                            recv_sem=recv.at[kind, n], device_id=device, device_id_type=MESH)

    def pair(src, dst, send_sem, recv_sem, device):
        return pltpu.make_async_remote_copy(src_ref=src, dst_ref=dst, send_sem=send_sem, recv_sem=recv_sem,
                                            device_id=device, device_id_type=MESH)

    def by_half(n, act_on):
        if isinstance(n, int):
            act_on(z0.at[n] if n < steps else z2.at[n - steps])
            return

        @pl.when(n < steps)
        def _():
            act_on(z0.at[n])

        @pl.when(n >= steps)
        def _():
            act_on(z2.at[n - steps])

    def go_row(n):
        return pair(ls.at[n - steps], z2.at[n - steps], send.at[0, n], recv.at[0, n], other(step_of(n)))

    def go_chip(n, src=None):
        src = z0.at[0] if src is None else src
        return pair(src.at[far], zy.at[n], send.at[1, n], recv.at[1, n], chip)

    def start_chip(n):
        by_half(n, lambda src: go_chip(n, src).start())

    def go_core(n, i, src=None):
        src = zy.at[n] if i == 0 else (z0.at[0] if src is None else src).at[near]
        return pair(src, zk.at[n, i], ksend.at[n, i], krecv.at[n, i], core)

    def start_core(n):
        go_core(n, 0).start()
        by_half(n, lambda src: go_core(n, 1, src).start())

    def go_expert(n):
        return remote(eo, ei, 2, n, core)

    def go_part(n):
        return remote(po, pi, 3, n, chip)

    def go_sum(n):
        return remote(sr, rr, 4, n, other(-step_of(n)))

    def local(src, dst, k):
        return pltpu.make_async_copy(src, dst, lsem.at[k])

    def run(*copies):
        for c in copies:
            c.start()
        for c in copies:
            c.wait()

    def weights(e, s):
        cs = []
        for i in range(fb):
            for o, w in enumerate((w1, w3)):
                cs.append(pltpu.make_async_copy(w.at[e, :, pl.ds(i * LANES, LANES)],
                                                w13b.at[s, :, pl.ds((2 * i + o) * LANES, LANES)],
                                                wsem.at[s, 2 * i + o]))
        cs.append(pltpu.make_async_copy(w2.at[e], w2b.at[s], wsem.at[s, 2 * fb]))
        return cs

    def hot(at, n):
        return lax.broadcasted_iota(I32, (n, at.shape[-1]), 0) == at

    barrier = pltpu.get_barrier_semaphore()
    partners = [core, chip] + [other(r) for r in range(1, steps)]
    for p in partners:
        pl.semaphore_signal(barrier, inc=1, device_id=p, device_id_type=MESH)
    for e in range(2):
        for c in weights(e, e):
            c.start()
    pl.semaphore_wait(barrier, len(partners))

    start_chip(0)
    run(local(z1, zin, 0))
    for i, r in enumerate(STEPS[1]):
        n = steps + i
        put = local(zb.at[i % 2], (z2 if r == 0 else ls).at[i], 1 + i % 2)
        sel = jnp.where(hot(lists[r:r + 1, :], width), 1.0, 0.0).astype(BF16)
        for c in range(4):
            cols = slice(c * quarter, (c + 1) * quarter)
            zb[i % 2, :, cols] = jnp.dot(sel, zin[:, cols], preferred_element_type=F32).astype(BF16)
        run(put)
        if r:
            go_row(n).start()
        if i == 0:
            go_chip(0).wait_recv()
            start_core(0)
            start_chip(1)

    def dispatch(n):
        @pl.when(n + 1 < nb)
        def _():
            go_chip(n + 1).wait_recv()
            start_core(n + 1)

        @pl.when(n + 2 < nb)
        def _():
            @pl.when(jnp.logical_and(n + 2 >= steps, step_of(n + 2) != 0))
            def _():
                go_row(n + 2).wait_recv()
            start_chip(n + 2)

    def experts(n):
        for i in range(2):
            go_core(n, i).wait_recv()
        srcs = (zk.at[n, 0], zk.at[n, 1], zy.at[n])
        fetch = lambda i, src: local(src, zb.at[i % 2, pl.ds(0, window)], 1 + i % 2)
        fetch(0, srcs[0]).start()
        for i in range(4):
            if i + 1 < 3:
                fetch(i + 1, srcs[i + 1]).start()
            elif i + 1 == 3:
                by_half(n, lambda src: fetch(3, src.at[near]).start())
            fetch(i, srcs[min(i, 2)]).wait()
            sel = jnp.concatenate([jnp.where(hot(px[n, i * el + e:i * el + e + 1, :], cap), 1.0, 0.0).astype(BF16)
                                   for e in range(el)], 0)
            for c in range(4):
                cols = slice(c * quarter, (c + 1) * quarter)
                v = jnp.dot(sel, zb[i % 2, 0:window, cols], preferred_element_type=F32).astype(BF16)
                for e in range(el):
                    x[e * rows + i * cap:e * rows + (i + 1) * cap, cols] = v[e * cap:(e + 1) * cap]

        def put(e, i):
            return pltpu.make_async_copy(x.at[pl.ds(pl.multiple_of(e * rows + i * cap, 32), cap)],
                                         (eo if i < 2 else em).at[n, i % 2, pl.ds(pl.multiple_of(e * cap, 32), cap)],
                                         psem.at[e, i])

        def expert(e, carry):
            s = lax.rem(e, 2)
            for c in weights(e, s):
                c.wait()

            def tile(k, cc):
                at = pl.ds(pl.multiple_of(e * rows + k * TILE, 32), TILE)
                for c in range(fb):
                    v = jnp.dot(x[at, :], w13b[s, :, 2 * c * LANES:2 * (c + 1) * LANES], preferred_element_type=F32)
                    act[:, c * LANES:(c + 1) * LANES] = (jax.nn.silu(v[:, :LANES]) * v[:, LANES:]).astype(BF16)
                for c in range(d // (2 * LANES)):
                    cols = slice(2 * c * LANES, 2 * (c + 1) * LANES)
                    x[at, cols] = jnp.dot(act[...], w2b[s, :, cols], preferred_element_type=F32).astype(BF16)
                return cc
            lax.fori_loop(0, rows // TILE, tile, 0)
            for i in range(4):
                put(e, i).start()

            @pl.when(n * el + e + 2 < nb * el)
            def _():
                for c in weights(lax.rem(e + 2, el), s):
                    c.start()
            return carry
        lax.fori_loop(0, el, expert, 0)
        for e in range(el):
            for i in range(4):
                put(e, i).wait()
        go_expert(n).start()

    def combine(n):
        go_expert(n).wait_recv()
        fetch = lambda i: (local(em.at[n, i], x.at[pl.ds(2 * i * rows, rows)], 1 + 2 * i),
                           local(ei.at[n, i], x.at[pl.ds((2 * i + 1) * rows, rows)], 2 + 2 * i))
        for i in range(2):
            for c in fetch(i):
                c.start()
        k = 2 * el
        for i in range(2):
            m = jnp.concatenate([jnp.where(hot(pb[n, i * k + e:i * k + e + 1, :], cap), gb[n, i * k + e:i * k + e + 1, :], 0.0)
                                 for e in range(k)], 0)
            parts = split3(m)
            for c in fetch(i):
                c.wait()
            for c in range(4):
                cols = slice(c * quarter, (c + 1) * quarter)
                b = x[2 * i * rows:2 * (i + 1) * rows, cols]
                a = [lax.dot_general(p, b, (((0,), (0,)), ((), ())), preferred_element_type=F32) for p in parts]
                ob[i, 0:window, cols] = a[0] + a[1] + a[2]
            put = local(ob.at[i, pl.ds(0, window)], (po, pm)[i].at[n], 5 + i)
            put.start()
            if i == 0:
                put.wait()
                go_part(n).start()
            else:
                put.wait()

    def forward(n):
        go_part(n).wait_recv()

        copies = (local(pm.at[n], ob.at[0, near], 1), local(pi.at[n], ob.at[1, far], 2))
        for c in copies:
            c.start()
        if gap:
            for i, first in enumerate((1 - col // 2, col // 2)):
                ob[i, pl.ds(pl.multiple_of(window * first, 16), gap), :] = jnp.zeros((gap, d), F32)
        for c in copies:
            c.wait()
        ob[0] = ob[0] + ob[1]
        run(local(ob.at[0], sr.at[n], 1))

        @pl.when(step_of(n) != 0)
        def _():
            go_sum(n).start()

    def finish(m):
        at = [m * steps + STEPS[m].index(r) for r in range(steps)]
        for r in range(1, steps):
            go_sum(at[r]).wait_recv()
        refs = [sr.at[at[0]]] + [rr.at[at[r]] for r in range(1, steps)]
        lane = lax.broadcasted_iota(I32, (t, width), 1)
        def pieces(c):
            return [local(a.at[:, pl.ds(c * quarter, quarter)], ob.at[c % 2, :, pl.ds(l * quarter, quarter)], 4 * (c % 2) + l)
                    for l, a in enumerate(refs)]

        for w in pieces(0):
            w.start()
        run(pltpu.make_async_copy(h[m], zin, psem.at[0, 0]))
        for c in range(4):
            cols = slice(c * quarter, (c + 1) * quarter)
            if c + 1 < 4:
                for w in pieces(c + 1):
                    w.start()
            for w in pieces(c):
                w.wait()
            v = zin[:, cols].astype(F32)
            for r in range(steps):
                one = jnp.where(lane == homes[m, :, r:r + 1], 1.0, 0.0).astype(BF16)
                for p in split3(ob[c % 2, :, r * quarter:(r + 1) * quarter]):
                    v = v + jnp.dot(one, p, preferred_element_type=F32)
            zin[:, cols] = v.astype(BF16)
        run(local(zin, y.at[m], 0))

    def block(n, carry):
        @pl.when(n < nb)
        def _():
            dispatch(n)
            experts(n)

        @pl.when(jnp.logical_and(n >= 1, n <= nb))
        def _():
            combine(n - 1)

        @pl.when(jnp.logical_and(n >= 2, n <= nb + 1))
        def _():
            forward(n - 2)

        @pl.when(n == nb - 1)
        def _():
            finish(0)

        @pl.when(n == nb + 2)
        def _():
            finish(1)
        return carry
    lax.fori_loop(0, nb + 3, block, 0)

    def drain(n, carry):
        for c in (go_chip(n), go_core(n, 0), go_core(n, 1), go_expert(n), go_part(n)):
            c.wait_send()

        @pl.when(step_of(n) != 0)
        def _():
            go_sum(n).wait_send()

            @pl.when(n >= steps)
            def _():
                go_row(n).wait_send()
        return carry
    lax.fori_loop(0, nb, drain, 0)


def solution(mesh):
    ep_axes = ("row", "col")
    tok_axes = ("dp", "row", "col")
    nrow, ncol = mesh.shape["row"], mesh.shape["col"]
    ep = nrow * ncol

    def local(x, idx, gates, wq, wk, wv, wo, gattn, gmoe, w1, w3, w2):
        nm, ns, seq, d = x.shape
        t = ns * seq
        top = idx.shape[-1]
        el, _, f = w1.shape
        n_exp = el * ep
        layer = n_exp // nrow
        cap = capacity(t, top, n_exp)
        row, col = lax.axis_index("row"), lax.axis_index("col")
        me = row * ncol + col
        chip, core = col // 2, col % 2

        pay = jnp.concatenate([idx.astype(F32), gates, jnp.zeros((nm, ns, seq, 16 - 2 * top), F32)], -1)
        pay = jnp.swapaxes(pay.reshape(nm, t, 16), 1, 2)
        every = lax.all_gather(pay, tok_axes)
        every = every.reshape((-1, ep) + every.shape[1:])

        def halves(idx_, first):
            half = layer // 2
            return [jnp.any(idx_ // half == 2 * first + c, -2) for c in range(2)]

        def width_needed(gap):
            need = 0
            for r in range(nrow):
                a, b = halves(every[:, :, :, :top].astype(I32), r)
                na, nb, both = (jnp.sum(v.astype(I32), -1) for v in (a & ~b, b & ~a, a & b))
                need = jnp.maximum(need, jnp.max(jnp.maximum(na, gap) + both + jnp.maximum(nb, gap)))
            return need

        def places_of(a, b, gap, width):
            only = [ranks(v) for v in (a & ~b, a & b, b & ~a)]
            na = jnp.sum((a & ~b).astype(I32), -1, keepdims=True)
            mid = jnp.maximum(na, gap)
            return jnp.where(a & b, mid + only[1], jnp.where(a, only[0], jnp.where(b, width - 1 - only[2], NONE)))

        mine = lax.dynamic_index_in_dim(jnp.swapaxes(every, 1, 2), lax.axis_index("dp"), 0, keepdims=False)

        def lists_of(m, width, window):
            steps = lax.rem(row + jnp.arange(nrow, dtype=I32), nrow)
            own = jnp.broadcast_to(idx[m].reshape(t, top).T[None], (nrow, top, t))
            return places_of(*halves(own, steps[:, None, None]), width - window, width)

        def layers(width, window, z0, h0, x):
            lists = [lists_of(m, width, window) for m in range(nm)]
            out = jax.ShapeDtypeStruct((width, d), BF16)
            rows0 = pl.pallas_call(
                list_kernel, out_shape=[out] * nrow, in_specs=[VMEM, VMEM], out_specs=[VMEM] * nrow, name="lists",
                compiler_params=pltpu.CompilerParams(vmem_limit_bytes=67043328),
                cost_estimate=pl.CostEstimate(flops=50_000_000, bytes_accessed=7_000_000, transcendentals=0),
            )(lists[0], z0)
            came = jnp.stack([rows0[r] if r == 0 else lax.ppermute(rows0[r], "row", [(i, (i + r) % nrow) for i in range(nrow)])
                              for r in STEPS[0]])
            x1, _ = lax.optimization_barrier((x[1], rows0[0]))
            h1, z1 = attention(x1.reshape(t, d), gattn, gmoe, wq, wk, wv, wo)
            homes = jnp.stack([jnp.pad(a.T, ((0, 0), (0, LANES - nrow))) for a in lists])
            nb = nm * nrow
            rows = el * cap
            table = jax.ShapeDtypeStruct((nb, 4 * el, window), I32)
            px, pb, gb = pl.pallas_call(
                functools.partial(routes_kernel, top, el, width - window),
                out_shape=[table, table, jax.ShapeDtypeStruct(table.shape, F32)],
                in_specs=[SMEM, VMEM], out_specs=[VMEM] * 3, scratch_shapes=[pltpu.VMEM((t, t), BF16)], name="routes",
                compiler_params=pltpu.CompilerParams(vmem_limit_bytes=67043328),
                cost_estimate=pl.CostEstimate(flops=50_000_000, bytes_accessed=2_000_000, transcendentals=0),
            )(jnp.stack([row, chip, core]).astype(I32), mine)
            wide = jax.ShapeDtypeStruct((nrow, width, d), BF16)
            part = jax.ShapeDtypeStruct((nb, window, d), F32)
            exact = jax.ShapeDtypeStruct((nb, width, d), F32)
            pair = jax.ShapeDtypeStruct((nb, 2, rows, d), BF16)
            y, *_ = pl.pallas_call(
                functools.partial(layer_kernel, cap, nrow),
                out_shape=[jax.ShapeDtypeStruct((nm, t, d), BF16), wide, wide, jax.ShapeDtypeStruct((nb, window, d), BF16),
                           jax.ShapeDtypeStruct((nb, 2, window, d), BF16), pair, pair, pair] + [part] * 3 + [exact] * 2,
                in_specs=[ANY] * 4 + [VMEM] * 5 + [ANY] * 3, out_specs=[ANY] * 13,
                scratch_shapes=[
                    pltpu.VMEM((t, d), BF16),
                    pltpu.VMEM((2, width, d), BF16),
                    pltpu.VMEM((4 * rows, d), BF16),
                    pltpu.VMEM((TILE, f), BF16),
                    pltpu.VMEM((2, d, 2 * f), BF16),
                    pltpu.VMEM((2, f, d), BF16),
                    pltpu.VMEM((2, width, d), F32),
                    pltpu.SemaphoreType.DMA((8,)),
                    pltpu.SemaphoreType.DMA((el, 4)),
                    pltpu.SemaphoreType.DMA((2, 2 * (f // LANES) + 1)),
                    pltpu.SemaphoreType.DMA((5, nb)),
                    pltpu.SemaphoreType.DMA((5, nb)),
                    pltpu.SemaphoreType.DMA((nb, 2)),
                    pltpu.SemaphoreType.DMA((nb, 2)),
                ],
                compiler_params=pltpu.CompilerParams(vmem_limit_bytes=67043328, has_side_effects=True,
                                                     collective_id=0 if width < t else 1),
                name="layer",
            )(came, z1, h0, h1, lists[1], homes, px, pb, gb, w1, w3, w2)
            return y.reshape(nm, ns, seq, d)

        h0, z0 = attention(x[0].reshape(t, d), gattn, gmoe, wq, wk, wv, wo)
        fits = width_needed(WIDTH - WINDOW) <= WIDTH
        return lax.cond(fits, functools.partial(layers, WIDTH, WINDOW), functools.partial(layers, t, t), z0, h0, x)

    tok_spec = P(None, tok_axes)
    exp_spec = P(ep_axes)
    return jax.shard_map(local, mesh=mesh,
                         in_specs=(tok_spec, tok_spec, tok_spec, P(), P(), P(), P(), P(), P(), exp_spec, exp_spec, exp_spec),
                         out_specs=tok_spec, check_vma=False)
```

```python
import functools

import jax
import jax.numpy as jnp
from jax import lax
from jax.experimental import pallas as pl
from jax.experimental.pallas import tpu as pltpu
from jax.sharding import PartitionSpec as P

HEAD = 128
LANES = 128
TILE = 384
WIDTH, WINDOW = 288, 208
NONE = -(1 << 20)
F32, BF16, I32 = jnp.float32, jnp.bfloat16, jnp.int32
ANY = pl.BlockSpec(memory_space=pl.ANY)
SMEM = pl.BlockSpec(memory_space=pltpu.SMEM)
VMEM = pl.BlockSpec(memory_space=pltpu.VMEM)
MESH = pl.DeviceIdType.MESH
STEPS = ((0, 1, 3, 2), (2, 3, 1, 0))


def rms(v, g):
    vf = v.astype(F32)
    return (vf * lax.rsqrt(jnp.mean(vf * vf, axis=-1, keepdims=True) + 1e-6) * g).astype(BF16)


def attention_kernel(x, ga, gm, wq, wk, wv, wo, h, z, u, acc):
    i = pl.program_id(0)
    t = x.shape[0]
    half = t // 2

    @pl.when(i == 0)
    def _():
        for c in range(4):
            rows = slice(c * t // 4, (c + 1) * t // 4)
            u[rows] = rms(x[rows], ga[...])
        acc[...] = jnp.zeros_like(acc)

    q, k, v = (jnp.dot(u[...], w[...], preferred_element_type=F32).astype(BF16) for w in (wq, wk, wv))
    heads = []
    for e in range(q.shape[1] // HEAD):
        cols = slice(e * HEAD, (e + 1) * HEAD)
        parts = []
        for b in range(2):
            keys = (b + 1) * half
            w = lax.dot_general(q[b * half:(b + 1) * half, cols], k[:keys, cols], (((1,), (1,)), ((), ())),
                                preferred_element_type=F32) * HEAD ** -0.5
            seen = (lax.broadcasted_iota(I32, (half, keys), 0) + b * half) >= lax.broadcasted_iota(I32, (half, keys), 1)
            w = jnp.where(seen, w, -1e30)
            p = jnp.exp(w - jnp.max(w, axis=1, keepdims=True))
            p = (p * (1.0 / jnp.sum(p, axis=1, keepdims=True))).astype(BF16)
            parts.append(jnp.dot(p, v[:keys, cols], preferred_element_type=F32).astype(BF16))
        heads.append(jnp.concatenate(parts, 0))
    acc[...] += jnp.dot(jnp.concatenate(heads, 1), wo[...], preferred_element_type=F32)

    @pl.when(i == pl.num_programs(0) - 1)
    def _():
        for c in range(4):
            rows = slice(c * t // 4, (c + 1) * t // 4)
            r = (x[rows].astype(F32) + acc[rows]).astype(BF16)
            h[rows] = r
            z[rows] = rms(r, gm[...])


def attention(x, ga, gm, wq, wk, wv, wo):
    t, d = x.shape
    step = 4 * HEAD
    whole = pl.BlockSpec((t, d), lambda i: (0, 0))
    gain = pl.BlockSpec((1, d), lambda i: (0, 0))
    down = pl.BlockSpec((d, step), lambda i: (0, i))
    out = jax.ShapeDtypeStruct((t, d), BF16)
    return pl.pallas_call(
        attention_kernel, grid=(wq.shape[1] // step,), out_shape=[out, out],
        in_specs=[whole, gain, gain, down, down, down, pl.BlockSpec((step, d), lambda i: (i, 0))],
        out_specs=[whole, whole], scratch_shapes=[pltpu.VMEM((t, d), BF16), pltpu.VMEM((t, d), F32)],
        compiler_params=pltpu.CompilerParams(vmem_limit_bytes=67043328), name="attention",
        cost_estimate=pl.CostEstimate(flops=200_000_000, bytes_accessed=40_000_000, transcendentals=0),
    )(x, ga[None], gm[None], wq, wk, wv, wo)


def capacity(t, top, n_exp):
    return ((top * ((2 * t + n_exp - 1) // n_exp) + 7) // 8) * 8


def split3(v):
    a = v.astype(BF16)
    r = v - a.astype(F32)
    b = r.astype(BF16)
    return a, b, (r - b.astype(F32)).astype(BF16)


def ranks(hit):
    t = hit.shape[-1]
    tri = (jnp.arange(t)[:, None] < jnp.arange(t)[None, :]).astype(BF16)
    n = jnp.dot(hit.reshape(-1, t).astype(BF16), tri, preferred_element_type=F32).astype(I32)
    return jnp.where(hit, n.reshape(hit.shape), NONE)


def among(idx, first, n):
    e = first + jnp.arange(n, dtype=I32)
    return idx[:, :, None, :] == e[None, None, :, None]


def routes_kernel(top, el, gap, spot, pay, px, pb, gb, tri):
    nm, ep, _, t = pay.shape
    nb, _, window = px.shape
    steps = nb // nm
    row, chip, core = spot[0], spot[1], spot[2]
    tri[...] = jnp.where(lax.broadcasted_iota(I32, (t, t), 0) < lax.broadcasted_iota(I32, (t, t), 1), 1.0, 0.0).astype(BF16)
    per = 2 * el
    first = (row * 2 + chip) * per
    e = lax.broadcasted_iota(I32, (per, 1), 0)
    mine = (first + lax.rem(e + el * core, per)).astype(F32)
    edge = (row * 2 * per).astype(F32)
    for n in range(nb):
        m, r = n // steps, STEPS[n // steps][n % steps]

        def source(i, carry):
            far_core, far_chip = 1 - i // 2, 1 - lax.rem(i, 2)
            k = core + far_core - 2 * core * far_core
            y = chip + far_chip - 2 * chip * far_chip
            p = lax.rem(row - r + steps, steps) * 4 + y * 2 + k
            chosen = pay[m, p, 0:top, :]
            gate = pay[m, p, top:2 * top, :]
            hit = jnp.zeros((per, t), F32)
            g = jnp.zeros((per, t), F32)
            in_a = jnp.zeros((1, t), F32)
            in_b = jnp.zeros((1, t), F32)
            for j in range(top):
                c = chosen[j:j + 1, :]
                same = c == mine
                hit = hit + jnp.where(same, 1.0, 0.0)
                g = g + jnp.where(same, gate[j:j + 1, :], 0.0)
                in_a = jnp.maximum(in_a, jnp.where((c >= edge) & (c < edge + per), 1.0, 0.0))
                in_b = jnp.maximum(in_b, jnp.where((c >= edge + per) & (c < edge + 2 * per), 1.0, 0.0))
            both = in_a * in_b
            kinds = jnp.concatenate([in_a - both, both, in_b - both, jnp.zeros((5, t), F32)], 0)
            rank = jnp.dot(jnp.concatenate([hit, kinds], 0).astype(BF16), tri[...], preferred_element_type=F32)
            na = jnp.sum(in_a - both, axis=1, keepdims=True)
            place = jnp.where(both > 0, jnp.maximum(na, float(gap)) + rank[per + 1:per + 2],
                              jnp.where(in_a > 0, rank[per:per + 1],
                                        jnp.where(in_b > 0, window + gap - 1.0 - rank[per + 2:per + 3], float(NONE))))
            place = (place - (chip * gap).astype(F32)).astype(I32)
            one = jnp.where(lax.broadcasted_iota(I32, (window, t), 0) == place, 1.0, 0.0).astype(BF16)
            wanted = jnp.where(hit > 0, rank[0:per] + 1.0, 0.0).astype(BF16)
            cols = jnp.concatenate([wanted.astype(F32)] + [v.astype(F32) for v in split3(g)], 0).astype(BF16)
            rows = lax.dot_general(cols, one, (((1,), (1,)), ((), ())), preferred_element_type=F32)
            at = rows[0:per].astype(I32) - 1
            px[n, pl.ds(i * el, el), :] = at[0:el]

            @pl.when(i >= 2)
            def _():
                pb[n, pl.ds((i - 2) * per, per), :] = at
                gb[n, pl.ds((i - 2) * per, per), :] = rows[per:2 * per] + rows[2 * per:3 * per] + rows[3 * per:]
            return carry
        for i in range(4):
            source(i, 0)


def list_kernel(pos, z, *outs):
    width, d = outs[0].shape
    row = lax.broadcasted_iota(I32, (width, z.shape[0]), 0)
    for l, o in enumerate(outs):
        sel = jnp.where(row == pos[l:l + 1, :], 1.0, 0.0).astype(BF16)
        for c in range(4):
            cols = slice(c * d // 4, (c + 1) * d // 4)
            o[:, cols] = jnp.dot(sel, z[:, cols], preferred_element_type=F32).astype(BF16)


def layer_kernel(cap, steps, za, zb0, zc, zd, y0, k0, k1, z1, h0, h1, lists, homes, px, pb, gb, w1, w3, w2,
                 y, ls, z2, zy, zk, eo, em, ei, po, pm, pi, sr, rr,
                 zin, zb, x, act, w13b, w2b, ob, fa, lsem, psem, fsem, wsem, send, recv, ksend, krecv):
    el, d, f = w1.shape
    t, _ = z1.shape
    h = (h0, h1)
    nm = len(h)
    nb = steps * nm
    width, window = zb.shape[1], zy.shape[1]
    gap = width - window
    early = (za, zb0, zc)
    ne = len(early)
    turns = fa.shape[1] != width
    fa = ob if turns else fa
    rows = el * cap
    fb = f // LANES
    quarter = d // 4
    dp, row, col = lax.axis_index("dp"), lax.axis_index("row"), lax.axis_index("col")
    near = pl.ds(pl.multiple_of(gap * (col // 2), 16), window)
    far = pl.ds(pl.multiple_of(gap * (1 - col // 2), 16), window)
    core = (dp, row, col + 1 - 2 * lax.rem(col, 2))
    chip = (dp, row, col + 2 - 4 * (col // 2))

    def other(r):
        return (dp, lax.rem(row + r + steps, steps), col)

    def step_of(n):
        i = lax.rem(n, steps)
        i = i + (n // steps) * (steps - 1 - 2 * i)
        return lax.rem(i * (i + 1) // 2, steps)

    def remote(src, dst, kind, n, device):
        return pltpu.make_async_remote_copy(src_ref=src.at[n], dst_ref=dst.at[n], send_sem=send.at[kind, n],
                                            recv_sem=recv.at[kind, n], device_id=device, device_id_type=MESH)

    def pair(src, dst, send_sem, recv_sem, device):
        return pltpu.make_async_remote_copy(src_ref=src, dst_ref=dst, send_sem=send_sem, recv_sem=recv_sem,
                                            device_id=device, device_id_type=MESH)

    def arrived(n, act_on):
        if isinstance(n, int):
            act_on(early[n] if n < ne else z2.at[n - ne])
            return
        for j in range(ne):
            @pl.when(n == j)
            def _(j=j):
                act_on(early[j])

        @pl.when(n >= ne)
        def _():
            act_on(z2.at[n - ne])

    def go_row(n):
        src = z2.at[n - ne] if not isinstance(n, int) else zd if n < steps else ls.at[n - steps]
        return pair(src, z2.at[n - ne], send.at[0, n], recv.at[0, n], other(step_of(n)))

    def go_chip(n, src=None):
        src = za if src is None else src
        return pair(src.at[far], zy.at[n], send.at[1, n], recv.at[1, n], chip)

    def start_chip(n):
        arrived(n, lambda src: go_chip(n, src).start())

    def go_core(n, i, src=None):
        src = zy.at[n] if i == 0 else (za if src is None else src).at[near]
        return pair(src, zk.at[n, i], ksend.at[n, i], krecv.at[n, i], core)

    def start_core(n):
        go_core(n, 0).start()
        arrived(n, lambda src: go_core(n, 1, src).start())

    def go_expert(n):
        return remote(eo, ei, 2, n, core)

    def go_part(n):
        return remote(po, pi, 3, n, chip)

    def go_sum(n):
        return remote(sr, rr, 4, n, other(-step_of(n)))

    def local(src, dst, k):
        return pltpu.make_async_copy(src, dst, lsem.at[k])

    def run(*copies):
        for c in copies:
            c.start()
        for c in copies:
            c.wait()

    def weights(e, s):
        cs = []
        for i in range(fb):
            for o, w in enumerate((w1, w3)):
                cs.append(pltpu.make_async_copy(w.at[e, :, pl.ds(i * LANES, LANES)],
                                                w13b.at[s, :, pl.ds((2 * i + o) * LANES, LANES)],
                                                wsem.at[s, 2 * i + o]))
        cs.append(pltpu.make_async_copy(w2.at[e], w2b.at[s], wsem.at[s, 2 * fb]))
        return cs

    def hot(at, n):
        return lax.broadcasted_iota(I32, (n, at.shape[-1]), 0) == at

    barrier = pltpu.get_barrier_semaphore()
    partners = [core, chip] + [other(r) for r in range(1, steps)]
    for p in partners:
        pl.semaphore_signal(barrier, inc=1, device_id=p, device_id_type=MESH)
    for e in range(2):
        for c in weights(e, e):
            c.start()
    pl.semaphore_wait(barrier, len(partners))

    go_row(steps - 1).start()
    start_chip(1)
    run(local(z1, zin, 0))
    for i, r in enumerate(STEPS[1]):
        n = steps + i
        put = local(zb.at[i % 2], z2.at[n - ne] if r == 0 else ls.at[i], 1 + i % 2)
        sel = jnp.where(hot(lists[r:r + 1, :], width), 1.0, 0.0).astype(BF16)
        for c in range(4):
            cols = slice(c * quarter, (c + 1) * quarter)
            zb[i % 2, :, cols] = jnp.dot(sel, zin[:, cols], preferred_element_type=F32).astype(BF16)
        run(put)
        if r:
            go_row(n).start()

    def dispatch(n):
        @pl.when(n + 1 < nb)
        def _():
            go_chip(n + 1).wait_recv()
            start_core(n + 1)

        @pl.when(n + 2 < nb)
        def _():
            @pl.when(jnp.logical_and(n + 2 >= ne, step_of(n + 2) != 0))
            def _():
                go_row(n + 2).wait_recv()
            start_chip(n + 2)

    def experts(n):
        @pl.when(n > 0)
        def _():
            for i in range(2):
                go_core(n, i).wait_recv()

        def fetch(i, src):
            return local(src, zb.at[i % 2, pl.ds(0, window)], 1 + i % 2)

        def start(i):
            if i == 3:
                arrived(n, lambda src: fetch(3, src.at[near]).start())
                return

            @pl.when(n == 0)
            def _():
                fetch(i, (k0, k1, y0)[i]).start()

            @pl.when(n > 0)
            def _():
                fetch(i, (zk.at[n, 0], zk.at[n, 1], zy.at[n])[i]).start()
        start(0)
        for i in range(4):
            if i + 1 < 4:
                start(i + 1)
            fetch(i, y0).wait()
            sel = jnp.concatenate([jnp.where(hot(px[n, i * el + e:i * el + e + 1, :], cap), 1.0, 0.0).astype(BF16)
                                   for e in range(el)], 0)
            for c in range(4):
                cols = slice(c * quarter, (c + 1) * quarter)
                v = jnp.dot(sel, zb[i % 2, 0:window, cols], preferred_element_type=F32).astype(BF16)
                for e in range(el):
                    x[e * rows + i * cap:e * rows + (i + 1) * cap, cols] = v[e * cap:(e + 1) * cap]

        if not turns:
            @pl.when(n >= 3)
            def _():
                send_on(n - 3)

        def put(e, i):
            return pltpu.make_async_copy(x.at[pl.ds(pl.multiple_of(e * rows + i * cap, 32), cap)],
                                         (eo if i < 2 else em).at[n, i % 2, pl.ds(pl.multiple_of(e * cap, 32), cap)],
                                         psem.at[e, i])

        def expert(e, carry):
            s = lax.rem(e, 2)
            for c in weights(e, s):
                c.wait()

            def tile(k, cc):
                at = pl.ds(pl.multiple_of(e * rows + k * TILE, 32), TILE)
                for c in range(fb):
                    v = jnp.dot(x[at, :], w13b[s, :, 2 * c * LANES:2 * (c + 1) * LANES], preferred_element_type=F32)
                    act[:, c * LANES:(c + 1) * LANES] = (jax.nn.silu(v[:, :LANES]) * v[:, LANES:]).astype(BF16)
                for c in range(d // (2 * LANES)):
                    cols = slice(2 * c * LANES, 2 * (c + 1) * LANES)
                    x[at, cols] = jnp.dot(act[...], w2b[s, :, cols], preferred_element_type=F32).astype(BF16)
                return cc
            lax.fori_loop(0, rows // TILE, tile, 0)
            for i in range(4):
                put(e, i).start()

            @pl.when(n * el + e + 2 < nb * el)
            def _():
                for c in weights(lax.rem(e + 2, el), s):
                    c.start()
            return carry
        lax.fori_loop(0, el, expert, 0)
        for e in range(el):
            for i in range(4):
                put(e, i).wait()
        go_expert(n).start()

    def combine(n):
        go_expert(n).wait_recv()
        fetch = lambda i: (local(em.at[n, i], x.at[pl.ds(2 * i * rows, rows)], 1 + 2 * i),
                           local(ei.at[n, i], x.at[pl.ds((2 * i + 1) * rows, rows)], 2 + 2 * i))
        for i in range(2):
            for c in fetch(i):
                c.start()
        k = 2 * el
        for i in range(2):
            m = jnp.concatenate([jnp.where(hot(pb[n, i * k + e:i * k + e + 1, :], cap), gb[n, i * k + e:i * k + e + 1, :], 0.0)
                                 for e in range(k)], 0)
            parts = split3(m)
            for c in fetch(i):
                c.wait()
            for c in range(4):
                cols = slice(c * quarter, (c + 1) * quarter)
                b = x[2 * i * rows:2 * (i + 1) * rows, cols]
                a = [lax.dot_general(p, b, (((0,), (0,)), ((), ())), preferred_element_type=F32) for p in parts]
                ob[i, 0:window, cols] = a[0] + a[1] + a[2]
            put = local(ob.at[i, pl.ds(0, window)], (po, pm)[i].at[n], 5 + i)
            put.start()
            if i == 0:
                put.wait()
                go_part(n).start()
            else:
                put.wait()

    def adding(n):
        return (pltpu.make_async_copy(pm.at[n], fa.at[0, near], fsem.at[0]),
                pltpu.make_async_copy(pi.at[n], fa.at[1, far], fsem.at[1]))

    def summed(n):
        return pltpu.make_async_copy(fa.at[0], sr.at[n], fsem.at[2])

    def add_start(n):
        go_part(n).wait_recv()
        for c in adding(n):
            c.start()

    def add_end(n):
        if gap:
            for i, first in enumerate((1 - col // 2, col // 2)):
                fa[i, pl.ds(pl.multiple_of(window * first, 16), gap), :] = jnp.zeros((gap, d), F32)
        for c in adding(n):
            c.wait()
        fa[0] = fa[0] + fa[1]
        summed(n).start()

    def send_on(n):
        summed(n).wait()

        @pl.when(step_of(n) != 0)
        def _():
            go_sum(n).start()

    def finish(m):
        at = [m * steps + STEPS[m].index(r) for r in range(steps)]
        for r in range(1, steps):
            go_sum(at[r]).wait_recv()
        refs = [sr.at[at[0]]] + [rr.at[at[r]] for r in range(1, steps)]
        lane = lax.broadcasted_iota(I32, (t, width), 1)
        def pieces(c):
            return [local(a.at[:, pl.ds(c * quarter, quarter)], ob.at[c % 2, :, pl.ds(l * quarter, quarter)], 4 * (c % 2) + l)
                    for l, a in enumerate(refs)]

        for w in pieces(0):
            w.start()
        run(pltpu.make_async_copy(h[m], zin, psem.at[0, 0]))
        for c in range(4):
            cols = slice(c * quarter, (c + 1) * quarter)
            if c + 1 < 4:
                for w in pieces(c + 1):
                    w.start()
            for w in pieces(c):
                w.wait()
            v = zin[:, cols].astype(F32)
            for r in range(steps):
                one = jnp.where(lane == homes[m, :, r:r + 1], 1.0, 0.0).astype(BF16)
                for p in split3(ob[c % 2, :, r * quarter:(r + 1) * quarter]):
                    v = v + jnp.dot(one, p, preferred_element_type=F32)
            zin[:, cols] = v.astype(BF16)
        run(local(zin, y.at[m], 0))

    def block(n, carry):
        @pl.when(n < nb)
        def _():
            dispatch(n)
            experts(n)

        if not turns:
            @pl.when(n >= nb)
            def _():
                send_on(n - 3)

            @pl.when(jnp.logical_and(n >= 2, n <= nb + 1))
            def _():
                add_start(n - 2)

        @pl.when(jnp.logical_and(n >= 1, n <= nb))
        def _():
            combine(n - 1)

        @pl.when(jnp.logical_and(n >= 2, n <= nb + 1))
        def _():
            if turns:
                add_start(n - 2)
            add_end(n - 2)
            if turns:
                send_on(n - 2)

        @pl.when(n == nb - 1)
        def _():
            finish(0)

        @pl.when(n == nb + 2)
        def _():
            finish(1)
        return carry
    lax.fori_loop(0, nb + 3, block, 0)

    def drain(n, carry):
        for c in (go_expert(n), go_part(n)):
            c.wait_send()

        @pl.when(n > 0)
        def _():
            for c in (go_chip(n), go_core(n, 0), go_core(n, 1)):
                c.wait_send()

        @pl.when(step_of(n) != 0)
        def _():
            go_sum(n).wait_send()

            @pl.when(n >= ne)
            def _():
                go_row(n).wait_send()
        return carry
    lax.fori_loop(0, nb, drain, 0)


def solution(mesh):
    ep_axes = ("row", "col")
    tok_axes = ("dp", "row", "col")
    nrow, ncol = mesh.shape["row"], mesh.shape["col"]
    ep = nrow * ncol

    def local(x, idx, gates, wq, wk, wv, wo, gattn, gmoe, w1, w3, w2):
        nm, ns, seq, d = x.shape
        t = ns * seq
        top = idx.shape[-1]
        el, _, f = w1.shape
        n_exp = el * ep
        layer = n_exp // nrow
        cap = capacity(t, top, n_exp)
        row, col = lax.axis_index("row"), lax.axis_index("col")
        me = row * ncol + col
        chip, core = col // 2, col % 2

        pay = jnp.concatenate([idx.astype(F32), gates, jnp.zeros((nm, ns, seq, 16 - 2 * top), F32)], -1)
        pay = jnp.swapaxes(pay.reshape(nm, t, 16), 1, 2)
        every = lax.all_gather(pay, tok_axes)
        every = every.reshape((-1, ep) + every.shape[1:])

        def halves(idx_, first):
            half = layer // 2
            return [jnp.any(idx_ // half == 2 * first + c, -2) for c in range(2)]

        def width_needed(gap):
            need = 0
            for r in range(nrow):
                a, b = halves(every[:, :, :, :top].astype(I32), r)
                na, nb, both = (jnp.sum(v.astype(I32), -1) for v in (a & ~b, b & ~a, a & b))
                need = jnp.maximum(need, jnp.max(jnp.maximum(na, gap) + both + jnp.maximum(nb, gap)))
            return need

        def places_of(a, b, gap, width):
            only = [ranks(v) for v in (a & ~b, a & b, b & ~a)]
            na = jnp.sum((a & ~b).astype(I32), -1, keepdims=True)
            mid = jnp.maximum(na, gap)
            return jnp.where(a & b, mid + only[1], jnp.where(a, only[0], jnp.where(b, width - 1 - only[2], NONE)))

        mine = lax.dynamic_index_in_dim(jnp.swapaxes(every, 1, 2), lax.axis_index("dp"), 0, keepdims=False)

        def lists_of(m, width, window):
            steps = lax.rem(row + jnp.arange(nrow, dtype=I32), nrow)
            own = jnp.broadcast_to(idx[m].reshape(t, top).T[None], (nrow, top, t))
            return places_of(*halves(own, steps[:, None, None]), width - window, width)

        def layers(width, window, z0, h0, x):
            lists = [lists_of(m, width, window) for m in range(nm)]
            out = jax.ShapeDtypeStruct((width, d), BF16)
            rows0 = pl.pallas_call(
                list_kernel, out_shape=[out] * nrow, in_specs=[VMEM, VMEM], out_specs=[VMEM] * nrow, name="lists",
                compiler_params=pltpu.CompilerParams(vmem_limit_bytes=67043328),
                cost_estimate=pl.CostEstimate(flops=50_000_000, bytes_accessed=7_000_000, transcendentals=0),
            )(lists[0], z0)
            gap = width - window
            came = [rows0[r] if r == 0 else lax.ppermute(rows0[r], "row", [(i, (i + r) % nrow) for i in range(nrow)])
                    for r in STEPS[0][:3]]
            part_of = lambda c: lax.dynamic_slice_in_dim(rows0[0], gap * c, window)
            y0 = lax.ppermute(part_of(1 - chip), "col", [(i, (i + 2) % ncol) for i in range(ncol)])
            k0, k1 = (lax.ppermute(a, "col", [(i, i + 1 - 2 * (i % 2)) for i in range(ncol)]) for a in (y0, part_of(chip)))
            x1, _ = lax.optimization_barrier((x[1], rows0[0]))
            h1, z1 = attention(x1.reshape(t, d), gattn, gmoe, wq, wk, wv, wo)
            homes = jnp.stack([jnp.pad(a.T, ((0, 0), (0, LANES - nrow))) for a in lists])
            nb = nm * nrow
            rows = el * cap
            table = jax.ShapeDtypeStruct((nb, 4 * el, window), I32)
            px, pb, gb = pl.pallas_call(
                functools.partial(routes_kernel, top, el, width - window),
                out_shape=[table, table, jax.ShapeDtypeStruct(table.shape, F32)],
                in_specs=[SMEM, VMEM], out_specs=[VMEM] * 3, scratch_shapes=[pltpu.VMEM((t, t), BF16)], name="routes",
                compiler_params=pltpu.CompilerParams(vmem_limit_bytes=67043328),
                cost_estimate=pl.CostEstimate(flops=50_000_000, bytes_accessed=2_000_000, transcendentals=0),
            )(jnp.stack([row, chip, core]).astype(I32), mine)
            wide = jax.ShapeDtypeStruct((nrow, width, d), BF16)
            late = jax.ShapeDtypeStruct((nb - 3, width, d), BF16)
            part = jax.ShapeDtypeStruct((nb, window, d), F32)
            exact = jax.ShapeDtypeStruct((nb, width, d), F32)
            pair = jax.ShapeDtypeStruct((nb, 2, rows, d), BF16)
            y, *_ = pl.pallas_call(
                functools.partial(layer_kernel, cap, nrow),
                out_shape=[jax.ShapeDtypeStruct((nm, t, d), BF16), wide, late, jax.ShapeDtypeStruct((nb, window, d), BF16),
                           jax.ShapeDtypeStruct((nb, 2, window, d), BF16), pair, pair, pair] + [part] * 3 + [exact] * 2,
                in_specs=[ANY] * 10 + [VMEM] * 5 + [ANY] * 3, out_specs=[ANY] * 13,
                scratch_shapes=[
                    pltpu.VMEM((t, d), BF16),
                    pltpu.VMEM((2, width, d), BF16),
                    pltpu.VMEM((4 * rows, d), BF16),
                    pltpu.VMEM((TILE, f), BF16),
                    pltpu.VMEM((2, d, 2 * f), BF16),
                    pltpu.VMEM((2, f, d), BF16),
                    pltpu.VMEM((2, width, d), F32),
                    pltpu.VMEM((2, width if window < width else 16, d), F32),
                    pltpu.SemaphoreType.DMA((8,)),
                    pltpu.SemaphoreType.DMA((el, 4)),
                    pltpu.SemaphoreType.DMA((3,)),
                    pltpu.SemaphoreType.DMA((2, 2 * (f // LANES) + 1)),
                    pltpu.SemaphoreType.DMA((5, nb)),
                    pltpu.SemaphoreType.DMA((5, nb)),
                    pltpu.SemaphoreType.DMA((nb, 2)),
                    pltpu.SemaphoreType.DMA((nb, 2)),
                ],
                compiler_params=pltpu.CompilerParams(vmem_limit_bytes=67043328, has_side_effects=True,
                                                     collective_id=0 if width < t else 1),
                name="layer",
            )(*came, rows0[STEPS[0][3]], y0, k0, k1, z1, h0, h1, lists[1], homes, px, pb, gb, w1, w3, w2)
            return y.reshape(nm, ns, seq, d)

        h0, z0 = attention(x[0].reshape(t, d), gattn, gmoe, wq, wk, wv, wo)
        fits = width_needed(WIDTH - WINDOW) <= WIDTH
        return lax.cond(fits, functools.partial(layers, WIDTH, WINDOW), functools.partial(layers, t, t), z0, h0, x)

    tok_spec = P(None, tok_axes)
    exp_spec = P(ep_axes)
    return jax.shard_map(local, mesh=mesh,
                         in_specs=(tok_spec, tok_spec, tok_spec, P(), P(), P(), P(), P(), P(), exp_spec, exp_spec, exp_spec),
                         out_specs=tok_spec, check_vma=False)
```

```python
import functools

import jax
import jax.numpy as jnp
from jax import lax
from jax.experimental import pallas as pl
from jax.experimental.pallas import tpu as pltpu
from jax.sharding import PartitionSpec as P

HEAD = 128
LANES = 128
TILE = 384
WIDTH, WINDOW = 288, 208
NONE = -(1 << 20)
F32, BF16, I32 = jnp.float32, jnp.bfloat16, jnp.int32
ANY = pl.BlockSpec(memory_space=pl.ANY)
SMEM = pl.BlockSpec(memory_space=pltpu.SMEM)
VMEM = pl.BlockSpec(memory_space=pltpu.VMEM)
MESH = pl.DeviceIdType.MESH
STEPS = ((1, 3, 2, 0), (2, 3, 1, 0))


def rms(v, g):
    vf = v.astype(F32)
    return (vf * lax.rsqrt(jnp.mean(vf * vf, axis=-1, keepdims=True) + 1e-6) * g).astype(BF16)


def attention_kernel(x, ga, gm, wq, wk, wv, wo, h, z, u, acc):
    i = pl.program_id(0)
    t = x.shape[0]
    half = t // 2

    @pl.when(i == 0)
    def _():
        for c in range(4):
            rows = slice(c * t // 4, (c + 1) * t // 4)
            u[rows] = rms(x[rows], ga[...])
        acc[...] = jnp.zeros_like(acc)

    q, k, v = (jnp.dot(u[...], w[...], preferred_element_type=F32).astype(BF16) for w in (wq, wk, wv))
    heads = []
    for e in range(q.shape[1] // HEAD):
        cols = slice(e * HEAD, (e + 1) * HEAD)
        parts = []
        for b in range(2):
            keys = (b + 1) * half
            w = lax.dot_general(q[b * half:(b + 1) * half, cols], k[:keys, cols], (((1,), (1,)), ((), ())),
                                preferred_element_type=F32) * HEAD ** -0.5
            seen = (lax.broadcasted_iota(I32, (half, keys), 0) + b * half) >= lax.broadcasted_iota(I32, (half, keys), 1)
            w = jnp.where(seen, w, -1e30)
            p = jnp.exp(w - jnp.max(w, axis=1, keepdims=True))
            p = (p * (1.0 / jnp.sum(p, axis=1, keepdims=True))).astype(BF16)
            parts.append(jnp.dot(p, v[:keys, cols], preferred_element_type=F32).astype(BF16))
        heads.append(jnp.concatenate(parts, 0))
    acc[...] += jnp.dot(jnp.concatenate(heads, 1), wo[...], preferred_element_type=F32)

    @pl.when(i == pl.num_programs(0) - 1)
    def _():
        for c in range(4):
            rows = slice(c * t // 4, (c + 1) * t // 4)
            r = (x[rows].astype(F32) + acc[rows]).astype(BF16)
            h[rows] = r
            z[rows] = rms(r, gm[...])


def attention(x, ga, gm, wq, wk, wv, wo):
    t, d = x.shape
    step = 4 * HEAD
    whole = pl.BlockSpec((t, d), lambda i: (0, 0))
    gain = pl.BlockSpec((1, d), lambda i: (0, 0))
    down = pl.BlockSpec((d, step), lambda i: (0, i))
    out = jax.ShapeDtypeStruct((t, d), BF16)
    return pl.pallas_call(
        attention_kernel, grid=(wq.shape[1] // step,), out_shape=[out, out],
        in_specs=[whole, gain, gain, down, down, down, pl.BlockSpec((step, d), lambda i: (i, 0))],
        out_specs=[whole, whole], scratch_shapes=[pltpu.VMEM((t, d), BF16), pltpu.VMEM((t, d), F32)],
        compiler_params=pltpu.CompilerParams(vmem_limit_bytes=67043328), name="attention",
        cost_estimate=pl.CostEstimate(flops=200_000_000, bytes_accessed=40_000_000, transcendentals=0),
    )(x, ga[None], gm[None], wq, wk, wv, wo)


def capacity(t, top, n_exp):
    return ((top * ((2 * t + n_exp - 1) // n_exp) + 7) // 8) * 8


def split3(v):
    a = v.astype(BF16)
    r = v - a.astype(F32)
    b = r.astype(BF16)
    return a, b, (r - b.astype(F32)).astype(BF16)


def ranks(hit):
    t = hit.shape[-1]
    tri = (jnp.arange(t)[:, None] < jnp.arange(t)[None, :]).astype(BF16)
    n = jnp.dot(hit.reshape(-1, t).astype(BF16), tri, preferred_element_type=F32).astype(I32)
    return jnp.where(hit, n.reshape(hit.shape), NONE)


def among(idx, first, n):
    e = first + jnp.arange(n, dtype=I32)
    return idx[:, :, None, :] == e[None, None, :, None]


def routes_kernel(top, el, gap, spot, pay, px, pb, gb, tri):
    nm, ep, _, t = pay.shape
    nb, _, window = px.shape
    steps = nb // nm
    row, chip, core = spot[0], spot[1], spot[2]
    tri[...] = jnp.where(lax.broadcasted_iota(I32, (t, t), 0) < lax.broadcasted_iota(I32, (t, t), 1), 1.0, 0.0).astype(BF16)
    per = 2 * el
    first = (row * 2 + chip) * per
    e = lax.broadcasted_iota(I32, (per, 1), 0)
    mine = (first + lax.rem(e + el * core, per)).astype(F32)
    edge = (row * 2 * per).astype(F32)
    for n in range(nb):
        m, r = n // steps, STEPS[n // steps][n % steps]

        def source(i, carry):
            far_core, far_chip = 1 - i // 2, 1 - lax.rem(i, 2)
            k = core + far_core - 2 * core * far_core
            y = chip + far_chip - 2 * chip * far_chip
            p = lax.rem(row - r + steps, steps) * 4 + y * 2 + k
            chosen = pay[m, p, 0:top, :]
            gate = pay[m, p, top:2 * top, :]
            hit = jnp.zeros((per, t), F32)
            g = jnp.zeros((per, t), F32)
            in_a = jnp.zeros((1, t), F32)
            in_b = jnp.zeros((1, t), F32)
            for j in range(top):
                c = chosen[j:j + 1, :]
                same = c == mine
                hit = hit + jnp.where(same, 1.0, 0.0)
                g = g + jnp.where(same, gate[j:j + 1, :], 0.0)
                in_a = jnp.maximum(in_a, jnp.where((c >= edge) & (c < edge + per), 1.0, 0.0))
                in_b = jnp.maximum(in_b, jnp.where((c >= edge + per) & (c < edge + 2 * per), 1.0, 0.0))
            both = in_a * in_b
            kinds = jnp.concatenate([in_a - both, both, in_b - both, jnp.zeros((5, t), F32)], 0)
            rank = jnp.dot(jnp.concatenate([hit, kinds], 0).astype(BF16), tri[...], preferred_element_type=F32)
            na = jnp.sum(in_a - both, axis=1, keepdims=True)
            place = jnp.where(both > 0, jnp.maximum(na, float(gap)) + rank[per + 1:per + 2],
                              jnp.where(in_a > 0, rank[per:per + 1],
                                        jnp.where(in_b > 0, window + gap - 1.0 - rank[per + 2:per + 3], float(NONE))))
            place = (place - (chip * gap).astype(F32)).astype(I32)
            one = jnp.where(lax.broadcasted_iota(I32, (window, t), 0) == place, 1.0, 0.0).astype(BF16)
            wanted = jnp.where(hit > 0, rank[0:per] + 1.0, 0.0).astype(BF16)
            cols = jnp.concatenate([wanted.astype(F32)] + [v.astype(F32) for v in split3(g)], 0).astype(BF16)
            rows = lax.dot_general(cols, one, (((1,), (1,)), ((), ())), preferred_element_type=F32)
            at = rows[0:per].astype(I32) - 1
            px[n, pl.ds(i * el, el), :] = at[0:el]

            @pl.when(i >= 2)
            def _():
                pb[n, pl.ds((i - 2) * per, per), :] = at
                gb[n, pl.ds((i - 2) * per, per), :] = rows[per:2 * per] + rows[2 * per:3 * per] + rows[3 * per:]
            return carry
        for i in range(4):
            source(i, 0)


def list_kernel(pos, z, *outs):
    width, d = outs[0].shape
    row = lax.broadcasted_iota(I32, (width, z.shape[0]), 0)
    for l, o in enumerate(outs):
        sel = jnp.where(row == pos[l:l + 1, :], 1.0, 0.0).astype(BF16)
        for c in range(4):
            cols = slice(c * d // 4, (c + 1) * d // 4)
            o[:, cols] = jnp.dot(sel, z[:, cols], preferred_element_type=F32).astype(BF16)


def layer_kernel(cap, steps, za, zb0, zc, zd, z1, h0, h1, lists, homes, px, pb, gb, w1, w3, w2,
                 y, ls, z2, zy, zk, eo, em, ei, po, pm, pi, sr, rr,
                 zin, zb, x, act, w13b, w2b, ob, lsem, psem, fsem, wsem, send, recv, ksend, krecv):
    el, d, f = w1.shape
    t, _ = z1.shape
    h = (h0, h1)
    nm = len(h)
    nb = steps * nm
    width, window = zb.shape[1], zy.shape[1]
    gap = width - window
    early = {0: za, 1: zb0, 3: zc}
    rows = el * cap
    fb = f // LANES
    quarter = d // 4
    dp, row, col = lax.axis_index("dp"), lax.axis_index("row"), lax.axis_index("col")
    near = pl.ds(pl.multiple_of(gap * (col // 2), 16), window)
    far = pl.ds(pl.multiple_of(gap * (1 - col // 2), 16), window)
    core = (dp, row, col + 1 - 2 * lax.rem(col, 2))
    chip = (dp, row, col + 2 - 4 * (col // 2))

    def other(r):
        return (dp, lax.rem(row + r + steps, steps), col)

    def step_of(n):
        i = lax.rem(n, steps)
        k = lax.rem(i + 1, steps)
        i = k + (n // steps) * (steps - 1 - i - k)
        return lax.rem(i * (i + 1) // 2, steps)

    def remote(src, dst, kind, n, device):
        return pltpu.make_async_remote_copy(src_ref=src.at[n], dst_ref=dst.at[n], send_sem=send.at[kind, n],
                                            recv_sem=recv.at[kind, n], device_id=device, device_id_type=MESH)

    def pair(src, dst, send_sem, recv_sem, device):
        return pltpu.make_async_remote_copy(src_ref=src, dst_ref=dst, send_sem=send_sem, recv_sem=recv_sem,
                                            device_id=device, device_id_type=MESH)

    def arrived(n, act_on):
        if isinstance(n, int):
            act_on(early.get(n, z2.at[n]))
            return
        late = n >= 0
        for j, ref in early.items():
            late = jnp.logical_and(late, n != j)

            @pl.when(n == j)
            def _(ref=ref):
                act_on(ref)

        @pl.when(late)
        def _():
            act_on(z2.at[n])

    def go_row(n):
        src = z2.at[n] if not isinstance(n, int) else zd if n < steps else ls.at[n]
        return pair(src, z2.at[n], send.at[0, n], recv.at[0, n], other(step_of(n)))

    def go_chip(n, src=None):
        src = za if src is None else src
        return pair(src.at[far], zy.at[n], send.at[1, n], recv.at[1, n], chip)

    def start_chip(n):
        arrived(n, lambda src: go_chip(n, src).start())

    def go_core(n, i, src=None):
        src = zy.at[n] if i == 0 else (za if src is None else src).at[near]
        return pair(src, zk.at[n, i], ksend.at[n, i], krecv.at[n, i], core)

    def start_core(n):
        go_core(n, 0).start()
        arrived(n, lambda src: go_core(n, 1, src).start())

    def go_expert(n):
        return remote(eo, ei, 2, n, core)

    def go_part(n):
        return remote(po, pi, 3, n, chip)

    def go_sum(n):
        return remote(sr, rr, 4, n, other(-step_of(n)))

    def local(src, dst, k):
        return pltpu.make_async_copy(src, dst, lsem.at[k])

    def run(*copies):
        for c in copies:
            c.start()
        for c in copies:
            c.wait()

    def weights(e, s):
        cs = []
        for i in range(fb):
            for o, w in enumerate((w1, w3)):
                cs.append(pltpu.make_async_copy(w.at[e, :, pl.ds(i * LANES, LANES)],
                                                w13b.at[s, :, pl.ds((2 * i + o) * LANES, LANES)],
                                                wsem.at[s, 2 * i + o]))
        cs.append(pltpu.make_async_copy(w2.at[e], w2b.at[s], wsem.at[s, 2 * fb]))
        return cs

    def hot(at, n):
        return lax.broadcasted_iota(I32, (n, at.shape[-1]), 0) == at

    barrier = pltpu.get_barrier_semaphore()
    partners = [core, chip] + [other(r) for r in range(1, steps)]
    for p in partners:
        pl.semaphore_signal(barrier, inc=1, device_id=p, device_id_type=MESH)
    for e in range(2):
        for c in weights(e, e):
            c.start()
    pl.semaphore_wait(barrier, len(partners))

    start_chip(0)
    start_chip(1)
    go_row(2).start()
    run(local(z1, zin, 0))
    for i, r in enumerate(STEPS[1]):
        n = steps + i
        put = local(zb.at[i % 2], (z2 if r == 0 else ls).at[n], 1 + i % 2)
        sel = jnp.where(hot(lists[r:r + 1, :], width), 1.0, 0.0).astype(BF16)
        for c in range(4):
            cols = slice(c * quarter, (c + 1) * quarter)
            zb[i % 2, :, cols] = jnp.dot(sel, zin[:, cols], preferred_element_type=F32).astype(BF16)
        run(put)
        if r:
            go_row(n).start()
    go_chip(0).wait_recv()
    start_core(0)

    def dispatch(n):
        @pl.when(n + 1 < nb)
        def _():
            go_chip(n + 1).wait_recv()
            start_core(n + 1)

        @pl.when(n + 2 < nb)
        def _():
            @pl.when(step_of(n + 2) != 0)
            def _():
                go_row(n + 2).wait_recv()
            start_chip(n + 2)

    def experts(n):
        for i in range(2):
            go_core(n, i).wait_recv()

        def fetch(i, src):
            return local(src, zb.at[i % 2, pl.ds(0, window)], 1 + i % 2)

        def start(i):
            if i == 3:
                arrived(n, lambda src: fetch(3, src.at[near]).start())
            else:
                fetch(i, (zk.at[n, 0], zk.at[n, 1], zy.at[n])[i]).start()
        start(0)
        for i in range(4):
            if i + 1 < 4:
                start(i + 1)
            fetch(i, zy.at[n]).wait()
            sel = jnp.concatenate([jnp.where(hot(px[n, i * el + e:i * el + e + 1, :], cap), 1.0, 0.0).astype(BF16)
                                   for e in range(el)], 0)
            for c in range(4):
                cols = slice(c * quarter, (c + 1) * quarter)
                v = jnp.dot(sel, zb[i % 2, 0:window, cols], preferred_element_type=F32).astype(BF16)
                for e in range(el):
                    x[e * rows + i * cap:e * rows + (i + 1) * cap, cols] = v[e * cap:(e + 1) * cap]

        def put(e, i):
            return pltpu.make_async_copy(x.at[pl.ds(pl.multiple_of(e * rows + i * cap, 32), cap)],
                                         (eo if i < 2 else em).at[n, i % 2, pl.ds(pl.multiple_of(e * cap, 32), cap)],
                                         psem.at[e, i])

        def expert(e, carry):
            s = lax.rem(e, 2)
            for c in weights(e, s):
                c.wait()

            def tile(k, cc):
                at = pl.ds(pl.multiple_of(e * rows + k * TILE, 32), TILE)
                for c in range(fb):
                    v = jnp.dot(x[at, :], w13b[s, :, 2 * c * LANES:2 * (c + 1) * LANES], preferred_element_type=F32)
                    act[:, c * LANES:(c + 1) * LANES] = (jax.nn.silu(v[:, :LANES]) * v[:, LANES:]).astype(BF16)
                for c in range(d // (2 * LANES)):
                    cols = slice(2 * c * LANES, 2 * (c + 1) * LANES)
                    x[at, cols] = jnp.dot(act[...], w2b[s, :, cols], preferred_element_type=F32).astype(BF16)
                return cc
            lax.fori_loop(0, rows // TILE, tile, 0)
            for i in range(4):
                put(e, i).start()

            @pl.when(n * el + e + 2 < nb * el)
            def _():
                for c in weights(lax.rem(e + 2, el), s):
                    c.start()
            return carry
        lax.fori_loop(0, el, expert, 0)
        dispatch(n)

        @pl.when(n >= 1)
        def _():
            add_start(n - 1)
        for e in range(el):
            for i in range(4):
                put(e, i).wait()
        go_expert(n).start()

    def combine(n):
        fetch = lambda i: (local(em.at[n, i], x.at[pl.ds(2 * i * rows, rows)], 1 + 2 * i),
                           local(ei.at[n, i], x.at[pl.ds((2 * i + 1) * rows, rows)], 2 + 2 * i))
        for i in range(2):
            for c in fetch(i):
                c.start()
        k = 2 * el
        for i in range(2):
            m = jnp.concatenate([jnp.where(hot(pb[n, i * k + e:i * k + e + 1, :], cap), gb[n, i * k + e:i * k + e + 1, :], 0.0)
                                 for e in range(k)], 0)
            parts = split3(m)
            for c in fetch(i):
                c.wait()
            for c in range(4):
                cols = slice(c * quarter, (c + 1) * quarter)
                b = x[2 * i * rows:2 * (i + 1) * rows, cols]
                a = [lax.dot_general(p, b, (((0,), (0,)), ((), ())), preferred_element_type=F32) for p in parts]
                ob[i, 0:window, cols] = a[0] + a[1] + a[2]
            put = local(ob.at[i, pl.ds(0, window)], (po, pm)[i].at[n], 5 + i)
            put.start()
            if i == 0:
                put.wait()
                go_part(n).start()
            else:
                put.wait()

    def adding(n):
        return (pltpu.make_async_copy(pm.at[n], ob.at[0, near], fsem.at[0]),
                pltpu.make_async_copy(pi.at[n], ob.at[1, far], fsem.at[1]))

    def summed(n):
        return pltpu.make_async_copy(ob.at[0], sr.at[n], fsem.at[2])

    def add_start(n):
        go_part(n).wait_recv()
        for c in adding(n):
            c.start()

    def add_end(n):
        if gap:
            for i, first in enumerate((1 - col // 2, col // 2)):
                ob[i, pl.ds(pl.multiple_of(window * first, 16), gap), :] = jnp.zeros((gap, d), F32)
        for c in adding(n):
            c.wait()
        ob[0] = ob[0] + ob[1]
        summed(n).start()

    def send_on(n):
        summed(n).wait()

        @pl.when(step_of(n) != 0)
        def _():
            go_sum(n).start()

    def finish(m):
        at = [m * steps + STEPS[m].index(r) for r in range(steps)]
        for r in range(1, steps):
            go_sum(at[r]).wait_recv()
        refs = [sr.at[at[0]]] + [rr.at[at[r]] for r in range(1, steps)]
        lane = lax.broadcasted_iota(I32, (t, width), 1)
        def pieces(c):
            return [local(a.at[:, pl.ds(c * quarter, quarter)], ob.at[c % 2, :, pl.ds(l * quarter, quarter)], 4 * (c % 2) + l)
                    for l, a in enumerate(refs)]

        for w in pieces(0):
            w.start()
        run(pltpu.make_async_copy(h[m], zin, psem.at[0, 0]))
        for c in range(4):
            cols = slice(c * quarter, (c + 1) * quarter)
            if c + 1 < 4:
                for w in pieces(c + 1):
                    w.start()
            for w in pieces(c):
                w.wait()
            v = zin[:, cols].astype(F32)
            for r in range(steps):
                one = jnp.where(lane == homes[m, :, r:r + 1], 1.0, 0.0).astype(BF16)
                for p in split3(ob[c % 2, :, r * quarter:(r + 1) * quarter]):
                    v = v + jnp.dot(one, p, preferred_element_type=F32)
            zin[:, cols] = v.astype(BF16)
        run(local(zin, y.at[m], 0))

    def block(n, carry):
        @pl.when(n < nb)
        def _():
            experts(n)

        @pl.when(n == nb)
        def _():
            add_start(n - 1)

        @pl.when(n >= 1)
        def _():
            add_end(n - 1)

        @pl.when(n < nb)
        def _():
            go_expert(n).wait_recv()

        @pl.when(n >= 1)
        def _():
            send_on(n - 1)

        @pl.when(n < nb)
        def _():
            combine(n)

        @pl.when(n == nb - 2)
        def _():
            finish(0)

        @pl.when(n == nb)
        def _():
            finish(1)
        return carry
    lax.fori_loop(0, nb + 1, block, 0)

    def drain(n, carry):
        for c in (go_chip(n), go_core(n, 0), go_core(n, 1), go_expert(n), go_part(n)):
            c.wait_send()

        @pl.when(step_of(n) != 0)
        def _():
            go_sum(n).wait_send()

            @pl.when(n >= 2)
            def _():
                go_row(n).wait_send()
        return carry
    lax.fori_loop(0, nb, drain, 0)


def solution(mesh):
    ep_axes = ("row", "col")
    tok_axes = ("dp", "row", "col")
    nrow, ncol = mesh.shape["row"], mesh.shape["col"]
    ep = nrow * ncol

    def local(x, idx, gates, wq, wk, wv, wo, gattn, gmoe, w1, w3, w2):
        nm, ns, seq, d = x.shape
        t = ns * seq
        top = idx.shape[-1]
        el, _, f = w1.shape
        n_exp = el * ep
        layer = n_exp // nrow
        cap = capacity(t, top, n_exp)
        row, col = lax.axis_index("row"), lax.axis_index("col")
        me = row * ncol + col
        chip, core = col // 2, col % 2

        pay = jnp.concatenate([idx.astype(F32), gates, jnp.zeros((nm, ns, seq, 16 - 2 * top), F32)], -1)
        pay = jnp.swapaxes(pay.reshape(nm, t, 16), 1, 2)
        every = lax.all_gather(pay, tok_axes)
        every = every.reshape((-1, ep) + every.shape[1:])

        def halves(idx_, first):
            half = layer // 2
            return [jnp.any(idx_ // half == 2 * first + c, -2) for c in range(2)]

        def width_needed(gap):
            need = 0
            for r in range(nrow):
                a, b = halves(every[:, :, :, :top].astype(I32), r)
                na, nb, both = (jnp.sum(v.astype(I32), -1) for v in (a & ~b, b & ~a, a & b))
                need = jnp.maximum(need, jnp.max(jnp.maximum(na, gap) + both + jnp.maximum(nb, gap)))
            return need

        def places_of(a, b, gap, width):
            only = [ranks(v) for v in (a & ~b, a & b, b & ~a)]
            na = jnp.sum((a & ~b).astype(I32), -1, keepdims=True)
            mid = jnp.maximum(na, gap)
            return jnp.where(a & b, mid + only[1], jnp.where(a, only[0], jnp.where(b, width - 1 - only[2], NONE)))

        mine = lax.dynamic_index_in_dim(jnp.swapaxes(every, 1, 2), lax.axis_index("dp"), 0, keepdims=False)

        def lists_of(m, width, window):
            steps = lax.rem(row + jnp.arange(nrow, dtype=I32), nrow)
            own = jnp.broadcast_to(idx[m].reshape(t, top).T[None], (nrow, top, t))
            return places_of(*halves(own, steps[:, None, None]), width - window, width)

        def layers(width, window, z0, h0, x):
            lists = [lists_of(m, width, window) for m in range(nm)]
            out = jax.ShapeDtypeStruct((width, d), BF16)
            rows0 = pl.pallas_call(
                list_kernel, out_shape=[out] * nrow, in_specs=[VMEM, VMEM], out_specs=[VMEM] * nrow, name="lists",
                compiler_params=pltpu.CompilerParams(vmem_limit_bytes=67043328),
                cost_estimate=pl.CostEstimate(flops=50_000_000, bytes_accessed=7_000_000, transcendentals=0),
            )(lists[0], z0)
            came = [lax.ppermute(rows0[r], "row", [(i, (i + r) % nrow) for i in range(nrow)]) for r in STEPS[0][:2]]
            x1, _ = lax.optimization_barrier((x[1], rows0[0]))
            h1, z1 = attention(x1.reshape(t, d), gattn, gmoe, wq, wk, wv, wo)
            homes = jnp.stack([jnp.pad(a.T, ((0, 0), (0, LANES - nrow))) for a in lists])
            nb = nm * nrow
            rows = el * cap
            table = jax.ShapeDtypeStruct((nb, 4 * el, window), I32)
            px, pb, gb = pl.pallas_call(
                functools.partial(routes_kernel, top, el, width - window),
                out_shape=[table, table, jax.ShapeDtypeStruct(table.shape, F32)],
                in_specs=[SMEM, VMEM], out_specs=[VMEM] * 3, scratch_shapes=[pltpu.VMEM((t, t), BF16)], name="routes",
                compiler_params=pltpu.CompilerParams(vmem_limit_bytes=67043328),
                cost_estimate=pl.CostEstimate(flops=50_000_000, bytes_accessed=2_000_000, transcendentals=0),
            )(jnp.stack([row, chip, core]).astype(I32), mine)
            wide = jax.ShapeDtypeStruct((nb, width, d), BF16)
            part = jax.ShapeDtypeStruct((nb, window, d), F32)
            exact = jax.ShapeDtypeStruct((nb, width, d), F32)
            pair = jax.ShapeDtypeStruct((nb, 2, rows, d), BF16)
            y, *_ = pl.pallas_call(
                functools.partial(layer_kernel, cap, nrow),
                out_shape=[jax.ShapeDtypeStruct((nm, t, d), BF16), wide, wide, jax.ShapeDtypeStruct((nb, window, d), BF16),
                           jax.ShapeDtypeStruct((nb, 2, window, d), BF16), pair, pair, pair] + [part] * 3 + [exact] * 2,
                in_specs=[ANY] * 7 + [VMEM] * 5 + [ANY] * 3, out_specs=[ANY] * 13,
                scratch_shapes=[
                    pltpu.VMEM((t, d), BF16),
                    pltpu.VMEM((2, width, d), BF16),
                    pltpu.VMEM((4 * rows, d), BF16),
                    pltpu.VMEM((TILE, f), BF16),
                    pltpu.VMEM((2, d, 2 * f), BF16),
                    pltpu.VMEM((2, f, d), BF16),
                    pltpu.VMEM((2, width, d), F32),
                    pltpu.SemaphoreType.DMA((8,)),
                    pltpu.SemaphoreType.DMA((el, 4)),
                    pltpu.SemaphoreType.DMA((3,)),
                    pltpu.SemaphoreType.DMA((2, 2 * (f // LANES) + 1)),
                    pltpu.SemaphoreType.DMA((5, nb)),
                    pltpu.SemaphoreType.DMA((5, nb)),
                    pltpu.SemaphoreType.DMA((nb, 2)),
                    pltpu.SemaphoreType.DMA((nb, 2)),
                ],
                compiler_params=pltpu.CompilerParams(vmem_limit_bytes=67043328, has_side_effects=True,
                                                     collective_id=0 if width < t else 1),
                name="layer",
            )(*came, rows0[0], rows0[STEPS[0][2]], z1, h0, h1, lists[1], homes, px, pb, gb, w1, w3, w2)
            return y.reshape(nm, ns, seq, d)

        h0, z0 = attention(x[0].reshape(t, d), gattn, gmoe, wq, wk, wv, wo)
        fits = width_needed(WIDTH - WINDOW) <= WIDTH
        return lax.cond(fits, functools.partial(layers, WIDTH, WINDOW), functools.partial(layers, t, t), z0, h0, x)

    tok_spec = P(None, tok_axes)
    exp_spec = P(ep_axes)
    return jax.shard_map(local, mesh=mesh,
                         in_specs=(tok_spec, tok_spec, tok_spec, P(), P(), P(), P(), P(), P(), exp_spec, exp_spec, exp_spec),
                         out_specs=tok_spec, check_vma=False)
```

```python
import functools

import jax
import jax.numpy as jnp
from jax import lax
from jax.experimental import pallas as pl
from jax.experimental.pallas import tpu as pltpu
from jax.sharding import PartitionSpec as P

HEAD = 128
LANES = 128
TILE = 384
WIDTH, WINDOW = 288, 208
NONE = -(1 << 20)
F32, BF16, I32 = jnp.float32, jnp.bfloat16, jnp.int32
ANY = pl.BlockSpec(memory_space=pl.ANY)
SMEM = pl.BlockSpec(memory_space=pltpu.SMEM)
VMEM = pl.BlockSpec(memory_space=pltpu.VMEM)
MESH = pl.DeviceIdType.MESH
STEPS = ((1, 3, 2, 0), (2, 3, 1, 0))


def rms(v, g):
    vf = v.astype(F32)
    return (vf * lax.rsqrt(jnp.mean(vf * vf, axis=-1, keepdims=True) + 1e-6) * g).astype(BF16)


def attention_kernel(x, ga, gm, wq, wk, wv, wo, h, z, u, acc):
    i = pl.program_id(0)
    t = x.shape[0]
    half = t // 2

    @pl.when(i == 0)
    def _():
        for c in range(4):
            rows = slice(c * t // 4, (c + 1) * t // 4)
            u[rows] = rms(x[rows], ga[...])
        acc[...] = jnp.zeros_like(acc)

    q, k, v = (jnp.dot(u[...], w[...], preferred_element_type=F32).astype(BF16) for w in (wq, wk, wv))
    heads = []
    for e in range(q.shape[1] // HEAD):
        cols = slice(e * HEAD, (e + 1) * HEAD)
        parts = []
        for b in range(2):
            keys = (b + 1) * half
            w = lax.dot_general(q[b * half:(b + 1) * half, cols], k[:keys, cols], (((1,), (1,)), ((), ())),
                                preferred_element_type=F32) * HEAD ** -0.5
            seen = (lax.broadcasted_iota(I32, (half, keys), 0) + b * half) >= lax.broadcasted_iota(I32, (half, keys), 1)
            w = jnp.where(seen, w, -1e30)
            p = jnp.exp(w - jnp.max(w, axis=1, keepdims=True))
            p = (p * (1.0 / jnp.sum(p, axis=1, keepdims=True))).astype(BF16)
            parts.append(jnp.dot(p, v[:keys, cols], preferred_element_type=F32).astype(BF16))
        heads.append(jnp.concatenate(parts, 0))
    acc[...] += jnp.dot(jnp.concatenate(heads, 1), wo[...], preferred_element_type=F32)

    @pl.when(i == pl.num_programs(0) - 1)
    def _():
        for c in range(4):
            rows = slice(c * t // 4, (c + 1) * t // 4)
            r = (x[rows].astype(F32) + acc[rows]).astype(BF16)
            h[rows] = r
            z[rows] = rms(r, gm[...])


def attention(x, m, t, ga, gm, wq, wk, wv, wo):
    d = x.shape[1]
    step = 4 * HEAD
    whole = pl.BlockSpec((t, d), lambda i: (0, 0))
    taken = pl.BlockSpec((t, d), lambda i: (m, 0))
    gain = pl.BlockSpec((1, d), lambda i: (0, 0))
    down = pl.BlockSpec((d, step), lambda i: (0, i))
    out = jax.ShapeDtypeStruct((t, d), BF16)
    return pl.pallas_call(
        attention_kernel, grid=(wq.shape[1] // step,), out_shape=[out, out],
        in_specs=[taken, gain, gain, down, down, down, pl.BlockSpec((step, d), lambda i: (i, 0))],
        out_specs=[whole, whole], scratch_shapes=[pltpu.VMEM((t, d), BF16), pltpu.VMEM((t, d), F32)],
        compiler_params=pltpu.CompilerParams(vmem_limit_bytes=67043328), name="attention",
        cost_estimate=pl.CostEstimate(flops=200_000_000, bytes_accessed=40_000_000, transcendentals=0),
    )(x, ga[None], gm[None], wq, wk, wv, wo)


def capacity(t, top, n_exp):
    return ((top * ((2 * t + n_exp - 1) // n_exp) + 7) // 8) * 8


def split3(v):
    a = v.astype(BF16)
    r = v - a.astype(F32)
    b = r.astype(BF16)
    return a, b, (r - b.astype(F32)).astype(BF16)


def ranks(hit):
    t = hit.shape[-1]
    tri = (jnp.arange(t)[:, None] < jnp.arange(t)[None, :]).astype(BF16)
    n = jnp.dot(hit.reshape(-1, t).astype(BF16), tri, preferred_element_type=F32).astype(I32)
    return jnp.where(hit, n.reshape(hit.shape), NONE)


def among(idx, first, n):
    e = first + jnp.arange(n, dtype=I32)
    return idx[:, :, None, :] == e[None, None, :, None]


def routes_kernel(top, el, gap, spot, pay, px, pb, gb, tri):
    _, _, nm, _, t = pay.shape
    nb, _, window = px.shape
    steps = nb // nm
    row, chip, core, dp = spot[0], spot[1], spot[2], spot[3]
    tri[...] = jnp.where(lax.broadcasted_iota(I32, (t, t), 0) < lax.broadcasted_iota(I32, (t, t), 1), 1.0, 0.0).astype(BF16)
    per = 2 * el
    first = (row * 2 + chip) * per
    e = lax.broadcasted_iota(I32, (per, 1), 0)
    mine = (first + lax.rem(e + el * core, per)).astype(F32)
    edge = (row * 2 * per).astype(F32)
    for n in range(nb):
        m, r = n // steps, STEPS[n // steps][n % steps]

        def source(i, carry):
            far_core, far_chip = 1 - i // 2, 1 - lax.rem(i, 2)
            k = core + far_core - 2 * core * far_core
            y = chip + far_chip - 2 * chip * far_chip
            p = lax.rem(row - r + steps, steps) * 4 + y * 2 + k
            chosen = pay[dp, p, m, 0:top, :]
            gate = pay[dp, p, m, top:2 * top, :]
            hit = jnp.zeros((per, t), F32)
            g = jnp.zeros((per, t), F32)
            in_a = jnp.zeros((1, t), F32)
            in_b = jnp.zeros((1, t), F32)
            for j in range(top):
                c = chosen[j:j + 1, :]
                same = c == mine
                hit = hit + jnp.where(same, 1.0, 0.0)
                g = g + jnp.where(same, gate[j:j + 1, :], 0.0)
                in_a = jnp.maximum(in_a, jnp.where((c >= edge) & (c < edge + per), 1.0, 0.0))
                in_b = jnp.maximum(in_b, jnp.where((c >= edge + per) & (c < edge + 2 * per), 1.0, 0.0))
            both = in_a * in_b
            kinds = jnp.concatenate([in_a - both, both, in_b - both, jnp.zeros((5, t), F32)], 0)
            rank = jnp.dot(jnp.concatenate([hit, kinds], 0).astype(BF16), tri[...], preferred_element_type=F32)
            na = jnp.sum(in_a - both, axis=1, keepdims=True)
            place = jnp.where(both > 0, jnp.maximum(na, float(gap)) + rank[per + 1:per + 2],
                              jnp.where(in_a > 0, rank[per:per + 1],
                                        jnp.where(in_b > 0, window + gap - 1.0 - rank[per + 2:per + 3], float(NONE))))
            place = (place - (chip * gap).astype(F32)).astype(I32)
            one = jnp.where(lax.broadcasted_iota(I32, (window, t), 0) == place, 1.0, 0.0).astype(BF16)
            wanted = jnp.where(hit > 0, rank[0:per] + 1.0, 0.0).astype(BF16)
            cols = jnp.concatenate([wanted.astype(F32)] + [v.astype(F32) for v in split3(g)], 0).astype(BF16)
            rows = lax.dot_general(cols, one, (((1,), (1,)), ((), ())), preferred_element_type=F32)
            at = rows[0:per].astype(I32) - 1
            px[n, pl.ds(i * el, el), :] = at[0:el]

            @pl.when(i >= 2)
            def _():
                pb[n, pl.ds((i - 2) * per, per), :] = at
                gb[n, pl.ds((i - 2) * per, per), :] = rows[per:2 * per] + rows[2 * per:3 * per] + rows[3 * per:]
            return carry
        for i in range(4):
            source(i, 0)


def list_kernel(pos, z, *outs):
    width, d = outs[0].shape
    row = lax.broadcasted_iota(I32, (width, z.shape[0]), 0)
    for l, o in enumerate(outs):
        sel = jnp.where(row == pos[l:l + 1, :], 1.0, 0.0).astype(BF16)
        for c in range(4):
            cols = slice(c * d // 4, (c + 1) * d // 4)
            o[:, cols] = jnp.dot(sel, z[:, cols], preferred_element_type=F32).astype(BF16)


def layer_kernel(cap, steps, za, zb0, zc, zd, z1, h0, h1, lists, homes, px, pb, gb, w1, w3, w2,
                 y, ls, z2, zy, zk, eo, em, ei, po, pm, pi, sr, rr,
                 zin, zb, x, act, w13b, w2b, ob, lsem, psem, fsem, wsem, send, recv, ksend, krecv):
    el, d, f = w1.shape
    t, _ = z1.shape
    h = (h0, h1)
    nm = len(h)
    nb = steps * nm
    width, window = zb.shape[1], zy.shape[1]
    gap = width - window
    early = {0: za, 1: zb0, 3: zc}
    rows = el * cap
    fb = f // LANES
    quarter = d // 4
    dp, row, col = lax.axis_index("dp"), lax.axis_index("row"), lax.axis_index("col")
    near = pl.ds(pl.multiple_of(gap * (col // 2), 16), window)
    far = pl.ds(pl.multiple_of(gap * (1 - col // 2), 16), window)
    core = (dp, row, col + 1 - 2 * lax.rem(col, 2))
    chip = (dp, row, col + 2 - 4 * (col // 2))

    def other(r):
        return (dp, lax.rem(row + r + steps, steps), col)

    def step_of(n):
        i = lax.rem(n, steps)
        k = lax.rem(i + 1, steps)
        i = k + (n // steps) * (steps - 1 - i - k)
        return lax.rem(i * (i + 1) // 2, steps)

    def remote(src, dst, kind, n, device):
        return pltpu.make_async_remote_copy(src_ref=src.at[n], dst_ref=dst.at[n], send_sem=send.at[kind, n],
                                            recv_sem=recv.at[kind, n], device_id=device, device_id_type=MESH)

    def pair(src, dst, send_sem, recv_sem, device):
        return pltpu.make_async_remote_copy(src_ref=src, dst_ref=dst, send_sem=send_sem, recv_sem=recv_sem,
                                            device_id=device, device_id_type=MESH)

    def arrived(n, act_on):
        if isinstance(n, int):
            act_on(early.get(n, z2.at[n]))
            return
        late = n >= 0
        for j, ref in early.items():
            late = jnp.logical_and(late, n != j)

            @pl.when(n == j)
            def _(ref=ref):
                act_on(ref)

        @pl.when(late)
        def _():
            act_on(z2.at[n])

    def go_row(n):
        src = z2.at[n] if not isinstance(n, int) else zd if n < steps else ls.at[n]
        return pair(src, z2.at[n], send.at[0, n], recv.at[0, n], other(step_of(n)))

    def go_chip(n, src=None):
        src = za if src is None else src
        return pair(src.at[far], zy.at[n], send.at[1, n], recv.at[1, n], chip)

    def start_chip(n):
        arrived(n, lambda src: go_chip(n, src).start())

    def go_core(n, i, src=None):
        src = zy.at[n] if i == 0 else (za if src is None else src).at[near]
        return pair(src, zk.at[n, i], ksend.at[n, i], krecv.at[n, i], core)

    def start_core(n):
        go_core(n, 0).start()
        arrived(n, lambda src: go_core(n, 1, src).start())

    def go_expert(n):
        return remote(eo, ei, 2, n, core)

    def go_part(n):
        return remote(po, pi, 3, n, chip)

    def go_sum(n):
        return remote(sr, rr, 4, n, other(-step_of(n)))

    def local(src, dst, k):
        return pltpu.make_async_copy(src, dst, lsem.at[k])

    def run(*copies):
        for c in copies:
            c.start()
        for c in copies:
            c.wait()

    def weights(e, s):
        cs = []
        for i in range(fb):
            for o, w in enumerate((w1, w3)):
                cs.append(pltpu.make_async_copy(w.at[e, :, pl.ds(i * LANES, LANES)],
                                                w13b.at[s, :, pl.ds((2 * i + o) * LANES, LANES)],
                                                wsem.at[s, 2 * i + o]))
        cs.append(pltpu.make_async_copy(w2.at[e], w2b.at[s], wsem.at[s, 2 * fb]))
        return cs

    def hot(at, n):
        return lax.broadcasted_iota(I32, (n, at.shape[-1]), 0) == at

    barrier = pltpu.get_barrier_semaphore()
    partners = [core, chip] + [other(r) for r in range(1, steps)]
    for p in partners:
        pl.semaphore_signal(barrier, inc=1, device_id=p, device_id_type=MESH)
    for e in range(2):
        for c in weights(e, e):
            c.start()
    pl.semaphore_wait(barrier, len(partners))

    start_chip(0)
    start_chip(1)
    go_row(2).start()
    run(local(z1, zin, 0))
    for i, r in enumerate(STEPS[1]):
        n = steps + i
        put = local(zb.at[i % 2], (z2 if r == 0 else ls).at[n], 1 + i % 2)
        sel = jnp.where(hot(lists[r:r + 1, :], width), 1.0, 0.0).astype(BF16)
        for c in range(4):
            cols = slice(c * quarter, (c + 1) * quarter)
            zb[i % 2, :, cols] = jnp.dot(sel, zin[:, cols], preferred_element_type=F32).astype(BF16)
        run(put)
        if r:
            go_row(n).start()
    go_chip(0).wait_recv()
    start_core(0)

    def dispatch(n):
        @pl.when(n + 1 < nb)
        def _():
            go_chip(n + 1).wait_recv()
            start_core(n + 1)

        @pl.when(n + 2 < nb)
        def _():
            @pl.when(step_of(n + 2) != 0)
            def _():
                go_row(n + 2).wait_recv()
            start_chip(n + 2)

    def experts(n):
        for i in range(2):
            go_core(n, i).wait_recv()

        def fetch(i, src):
            return local(src, zb.at[i % 2, pl.ds(0, window)], 1 + i % 2)

        def start(i):
            if i == 3:
                arrived(n, lambda src: fetch(3, src.at[near]).start())
            else:
                fetch(i, (zk.at[n, 0], zk.at[n, 1], zy.at[n])[i]).start()
        start(0)
        for i in range(4):
            if i + 1 < 4:
                start(i + 1)
            fetch(i, zy.at[n]).wait()
            sel = jnp.concatenate([jnp.where(hot(px[n, i * el + e:i * el + e + 1, :], cap), 1.0, 0.0).astype(BF16)
                                   for e in range(el)], 0)
            for c in range(4):
                cols = slice(c * quarter, (c + 1) * quarter)
                v = jnp.dot(sel, zb[i % 2, 0:window, cols], preferred_element_type=F32).astype(BF16)
                for e in range(el):
                    x[e * rows + i * cap:e * rows + (i + 1) * cap, cols] = v[e * cap:(e + 1) * cap]

        def put(e, i):
            return pltpu.make_async_copy(x.at[pl.ds(pl.multiple_of(e * rows + i * cap, 32), cap)],
                                         (eo if i < 2 else em).at[n, i % 2, pl.ds(pl.multiple_of(e * cap, 32), cap)],
                                         psem.at[e, i])

        def expert(e, carry):
            s = lax.rem(e, 2)
            for c in weights(e, s):
                c.wait()

            def tile(k, cc):
                at = pl.ds(pl.multiple_of(e * rows + k * TILE, 32), TILE)
                for c in range(fb):
                    v = jnp.dot(x[at, :], w13b[s, :, 2 * c * LANES:2 * (c + 1) * LANES], preferred_element_type=F32)
                    act[:, c * LANES:(c + 1) * LANES] = (jax.nn.silu(v[:, :LANES]) * v[:, LANES:]).astype(BF16)
                for c in range(d // (2 * LANES)):
                    cols = slice(2 * c * LANES, 2 * (c + 1) * LANES)
                    x[at, cols] = jnp.dot(act[...], w2b[s, :, cols], preferred_element_type=F32).astype(BF16)
                return cc
            lax.fori_loop(0, rows // TILE, tile, 0)
            for i in range(4):
                put(e, i).start()

            @pl.when(n * el + e + 2 < nb * el)
            def _():
                for c in weights(lax.rem(e + 2, el), s):
                    c.start()
            return carry
        lax.fori_loop(0, el, expert, 0)
        dispatch(n)

        @pl.when(n >= 1)
        def _():
            add_start(n - 1)
        for e in range(el):
            for i in range(4):
                put(e, i).wait()
        go_expert(n).start()

    def combine(n):
        fetch = lambda i: (local(em.at[n, i], x.at[pl.ds(2 * i * rows, rows)], 1 + 2 * i),
                           local(ei.at[n, i], x.at[pl.ds((2 * i + 1) * rows, rows)], 2 + 2 * i))
        for i in range(2):
            for c in fetch(i):
                c.start()
        k = 2 * el
        for i in range(2):
            m = jnp.concatenate([jnp.where(hot(pb[n, i * k + e:i * k + e + 1, :], cap), gb[n, i * k + e:i * k + e + 1, :], 0.0)
                                 for e in range(k)], 0)
            parts = split3(m)
            for c in fetch(i):
                c.wait()
            for c in range(4):
                cols = slice(c * quarter, (c + 1) * quarter)
                b = x[2 * i * rows:2 * (i + 1) * rows, cols]
                a = [lax.dot_general(p, b, (((0,), (0,)), ((), ())), preferred_element_type=F32) for p in parts]
                ob[i, 0:window, cols] = a[0] + a[1] + a[2]
            put = local(ob.at[i, pl.ds(0, window)], (po, pm)[i].at[n], 5 + i)
            put.start()
            if i == 0:
                put.wait()
                go_part(n).start()
            else:
                put.wait()

    def adding(n):
        return (pltpu.make_async_copy(pm.at[n], ob.at[0, near], fsem.at[0]),
                pltpu.make_async_copy(pi.at[n], ob.at[1, far], fsem.at[1]))

    def summed(n):
        return pltpu.make_async_copy(ob.at[0], sr.at[n], fsem.at[2])

    def add_start(n):
        go_part(n).wait_recv()
        for c in adding(n):
            c.start()

    def add_end(n):
        if gap:
            for i, first in enumerate((1 - col // 2, col // 2)):
                ob[i, pl.ds(pl.multiple_of(window * first, 16), gap), :] = jnp.zeros((gap, d), F32)
        for c in adding(n):
            c.wait()
        ob[0] = ob[0] + ob[1]
        summed(n).start()

    def send_on(n):
        summed(n).wait()

        @pl.when(step_of(n) != 0)
        def _():
            go_sum(n).start()

    def finish(m):
        at = [m * steps + STEPS[m].index(r) for r in range(steps)]
        for r in range(1, steps):
            go_sum(at[r]).wait_recv()
        refs = [sr.at[at[0]]] + [rr.at[at[r]] for r in range(1, steps)]
        lane = lax.broadcasted_iota(I32, (t, width), 1)
        def pieces(c):
            return [local(a.at[:, pl.ds(c * quarter, quarter)], ob.at[c % 2, :, pl.ds(l * quarter, quarter)], 4 * (c % 2) + l)
                    for l, a in enumerate(refs)]

        for w in pieces(0):
            w.start()
        run(pltpu.make_async_copy(h[m], zin, psem.at[0, 0]))
        for c in range(4):
            cols = slice(c * quarter, (c + 1) * quarter)
            if c + 1 < 4:
                for w in pieces(c + 1):
                    w.start()
            for w in pieces(c):
                w.wait()
            v = zin[:, cols].astype(F32)
            for r in range(steps):
                one = jnp.where(lane == homes[m, :, r:r + 1], 1.0, 0.0).astype(BF16)
                for p in split3(ob[c % 2, :, r * quarter:(r + 1) * quarter]):
                    v = v + jnp.dot(one, p, preferred_element_type=F32)
            zin[:, cols] = v.astype(BF16)
        run(local(zin, y.at[m], 0))

    def block(n, carry):
        @pl.when(n < nb)
        def _():
            experts(n)

        @pl.when(n == nb)
        def _():
            add_start(n - 1)

        @pl.when(n >= 1)
        def _():
            add_end(n - 1)

        @pl.when(n < nb)
        def _():
            go_expert(n).wait_recv()

        @pl.when(n >= 1)
        def _():
            send_on(n - 1)

        @pl.when(n < nb)
        def _():
            combine(n)

        @pl.when(n == nb - 2)
        def _():
            finish(0)

        @pl.when(n == nb)
        def _():
            finish(1)
        return carry
    lax.fori_loop(0, nb + 1, block, 0)

    def drain(n, carry):
        for c in (go_chip(n), go_core(n, 0), go_core(n, 1), go_expert(n), go_part(n)):
            c.wait_send()

        @pl.when(step_of(n) != 0)
        def _():
            go_sum(n).wait_send()

            @pl.when(n >= 2)
            def _():
                go_row(n).wait_send()
        return carry
    lax.fori_loop(0, nb, drain, 0)


def solution(mesh):
    ep_axes = ("row", "col")
    tok_axes = ("dp", "row", "col")
    nrow, ncol = mesh.shape["row"], mesh.shape["col"]
    ep = nrow * ncol

    def local(x, idx, gates, wq, wk, wv, wo, gattn, gmoe, w1, w3, w2):
        nm, ns, seq, d = x.shape
        t = ns * seq
        top = idx.shape[-1]
        el, _, f = w1.shape
        n_exp = el * ep
        layer = n_exp // nrow
        cap = capacity(t, top, n_exp)
        row, col = lax.axis_index("row"), lax.axis_index("col")
        me = row * ncol + col
        chip, core = col // 2, col % 2

        def halves(idx_, first):
            half = layer // 2
            return [jnp.any(idx_ // half == 2 * first + c, -2) for c in range(2)]

        flat = x.reshape(nm * t, d)
        chosen = jnp.swapaxes(idx.reshape(nm, t, top), 1, 2)

        def width_needed(gap):
            a, b = halves(chosen[:, None], jnp.arange(nrow, dtype=I32)[:, None, None])
            na, nb, both = (jnp.sum(v.astype(I32), -1) for v in (a & ~b, b & ~a, a & b))
            return jnp.max(jnp.maximum(na, gap) + both + jnp.maximum(nb, gap))

        need = jnp.full((nm, 16 - 2 * top, t), width_needed(WIDTH - WINDOW), F32)
        pay = jnp.concatenate([chosen.astype(F32), jnp.swapaxes(gates.reshape(nm, t, top), 1, 2), need], 1)
        every = lax.all_gather(pay, tok_axes)
        every = every.reshape((-1, ep) + every.shape[1:])

        def places_of(a, b, gap, width):
            only = [ranks(v) for v in (a & ~b, a & b, b & ~a)]
            na = jnp.sum((a & ~b).astype(I32), -1, keepdims=True)
            mid = jnp.maximum(na, gap)
            return jnp.where(a & b, mid + only[1], jnp.where(a, only[0], jnp.where(b, width - 1 - only[2], NONE)))

        def lists_of(m, width, window):
            steps = lax.rem(row + jnp.arange(nrow, dtype=I32), nrow)
            own = jnp.broadcast_to(chosen[m][None], (nrow, top, t))
            return places_of(*halves(own, steps[:, None, None]), width - window, width)

        def layers(width, window, z0, h0, x, lists):
            out = jax.ShapeDtypeStruct((width, d), BF16)
            rows0 = pl.pallas_call(
                list_kernel, out_shape=[out] * nrow, in_specs=[VMEM, VMEM], out_specs=[VMEM] * nrow, name="lists",
                compiler_params=pltpu.CompilerParams(vmem_limit_bytes=67043328),
                cost_estimate=pl.CostEstimate(flops=50_000_000, bytes_accessed=7_000_000, transcendentals=0),
            )(lists[0], z0)
            came = [lax.ppermute(rows0[r], "row", [(i, (i + r) % nrow) for i in range(nrow)]) for r in STEPS[0][:2]]
            x1, _ = lax.optimization_barrier((x, rows0[0]))
            h1, z1 = attention(x1, 1, t, gattn, gmoe, wq, wk, wv, wo)
            homes = jnp.stack([jnp.pad(a.T, ((0, 0), (0, LANES - nrow))) for a in lists])
            nb = nm * nrow
            rows = el * cap
            table = jax.ShapeDtypeStruct((nb, 4 * el, window), I32)
            px, pb, gb = pl.pallas_call(
                functools.partial(routes_kernel, top, el, width - window),
                out_shape=[table, table, jax.ShapeDtypeStruct(table.shape, F32)],
                in_specs=[SMEM, VMEM], out_specs=[VMEM] * 3, scratch_shapes=[pltpu.VMEM((t, t), BF16)], name="routes",
                compiler_params=pltpu.CompilerParams(vmem_limit_bytes=67043328),
                cost_estimate=pl.CostEstimate(flops=50_000_000, bytes_accessed=2_000_000, transcendentals=0),
            )(jnp.stack([row, chip, core, lax.axis_index("dp")]).astype(I32), every)
            wide = jax.ShapeDtypeStruct((nb, width, d), BF16)
            part = jax.ShapeDtypeStruct((nb, window, d), F32)
            exact = jax.ShapeDtypeStruct((nb, width, d), F32)
            pair = jax.ShapeDtypeStruct((nb, 2, rows, d), BF16)
            y, *_ = pl.pallas_call(
                functools.partial(layer_kernel, cap, nrow),
                out_shape=[jax.ShapeDtypeStruct((nm, t, d), BF16), wide, wide, jax.ShapeDtypeStruct((nb, window, d), BF16),
                           jax.ShapeDtypeStruct((nb, 2, window, d), BF16), pair, pair, pair] + [part] * 3 + [exact] * 2,
                in_specs=[ANY] * 7 + [VMEM] * 5 + [ANY] * 3, out_specs=[ANY] * 13,
                scratch_shapes=[
                    pltpu.VMEM((t, d), BF16),
                    pltpu.VMEM((2, width, d), BF16),
                    pltpu.VMEM((4 * rows, d), BF16),
                    pltpu.VMEM((TILE, f), BF16),
                    pltpu.VMEM((2, d, 2 * f), BF16),
                    pltpu.VMEM((2, f, d), BF16),
                    pltpu.VMEM((2, width, d), F32),
                    pltpu.SemaphoreType.DMA((8,)),
                    pltpu.SemaphoreType.DMA((el, 4)),
                    pltpu.SemaphoreType.DMA((3,)),
                    pltpu.SemaphoreType.DMA((2, 2 * (f // LANES) + 1)),
                    pltpu.SemaphoreType.DMA((5, nb)),
                    pltpu.SemaphoreType.DMA((5, nb)),
                    pltpu.SemaphoreType.DMA((nb, 2)),
                    pltpu.SemaphoreType.DMA((nb, 2)),
                ],
                compiler_params=pltpu.CompilerParams(vmem_limit_bytes=67043328, has_side_effects=True,
                                                     collective_id=0 if width < t else 1),
                name="layer",
            )(*came, rows0[0], rows0[STEPS[0][2]], z1, h0, h1, lists[1], homes, px, pb, gb, w1, w3, w2)
            return y.reshape(nm, ns, seq, d)

        h0, z0 = attention(flat, 0, t, gattn, gmoe, wq, wk, wv, wo)
        fits = jnp.max(every[:, :, 0, 2 * top, 0]) <= WIDTH
        short, full = ([lists_of(m, *shape) for m in range(nm)] for shape in ((WIDTH, WINDOW), (t, t)))
        return lax.cond(fits, lambda z, h, x, a, b: layers(WIDTH, WINDOW, z, h, x, a),
                        lambda z, h, x, a, b: layers(t, t, z, h, x, b), z0, h0, flat, short, full)

    tok_spec = P(None, tok_axes)
    exp_spec = P(ep_axes)
    return jax.shard_map(local, mesh=mesh,
                         in_specs=(tok_spec, tok_spec, tok_spec, P(), P(), P(), P(), P(), P(), exp_spec, exp_spec, exp_spec),
                         out_specs=tok_spec, check_vma=False)
```
